32 devices in a mesh: rows: 4 (over y, core), cols: 8 (over z, x), hub: 1.
Axes of the slice: x: 2, y: 2, z: 4, core: 2. Of those that a mesh axis runs over, the one named last changes fastest.
Arguments:
- light_bits: int32 [96, 3072], P('rows', 'cols'), may hold values from -2147483648 to 2147483647, as said below
- hub_bits: int32 [4, 3072], P('hub', 'cols'), may hold values from -2147483648 to 2147483647, as said below
- hub_ids: int32 [128], replicated, may hold values from 0 to 3071, as said below
Outputs:
- clustering: float32 [3072], P(('rows', 'cols'))
The draws below stay inside these ranges and needn't reach their ends.
Inputs may be any that keep to these rules, and one draw needn't show every extreme that they name: Every word holds 32 bits; the matrix of light_bits is symmetric with a zero diagonal. `hub_bits`: every word holds 32 bits. `hub_ids`: 128 distinct vertex numbers.
All inputs are finite; a program needn't handle non-finite values.
Results may differ from the reference program's by a relative error of at most 0.0003.
Values sent between devices are 32-bit elements; how exact they have to be, the bound alone decides.
A program may use at most 128 MiB of HBM per device.

```python
import jax
import jax.numpy as jnp
from jax import lax

VERTICES = 3072
HUBS = 128


def vertex_weights(key):
    vertex_rank = jax.random.permutation(jax.random.fold_in(key, 7), VERTICES).astype(jnp.int32)
    weight = 4 + 128 // (1 + vertex_rank // 32)
    return (vertex_rank, weight)


def pack_bits(linked):
    powers = jnp.left_shift(jnp.int32(1), jnp.arange(32, dtype=jnp.int32))
    grouped = linked.astype(jnp.int32).reshape(linked.shape[0] // 32, 32, linked.shape[1])
    return jnp.sum(grouped * powers[None, :, None], axis=1).astype(jnp.int32)


def draw_light_bits(key, part):
    vertex_rank, weight = vertex_weights(key)
    samples = jax.random.randint(jax.random.fold_in(key, 11), (VERTICES, VERTICES), 0, 8192, dtype=jnp.int32)
    linked = samples < weight[:, None] * weight[None, :]
    vertex_ids = jnp.arange(VERTICES, dtype=jnp.int32)
    one_side = jnp.logical_and(linked, vertex_ids[None, :] > vertex_ids[:, None])
    symmetric = jnp.logical_or(one_side, one_side.T)
    return pack_bits(symmetric)


def draw_hub_bits(key, part):
    vertex_rank, weight = vertex_weights(key)
    samples = jax.random.randint(jax.random.fold_in(key, 13), (HUBS, VERTICES), 0, 1024, dtype=jnp.int32)
    linked = samples < 48 + weight[None, :]
    return pack_bits(linked)


def draw_hub_ids(key, part):
    vertex_rank, weight = vertex_weights(key)
    by_rank = jnp.argsort(vertex_rank)
    return by_rank[:HUBS].astype(jnp.int32)


def setup_inputs(seed: int = 0) -> dict:
    streams_of = jax.random.split(jax.random.key(seed), 4)
    return {
        "light_bits": draw_light_bits(jax.random.fold_in(streams_of[3], 71), 0),
        "hub_bits": draw_hub_bits(jax.random.fold_in(streams_of[3], 71), 0),
        "hub_ids": draw_hub_ids(jax.random.fold_in(streams_of[3], 71), 0),
    }


def unpack(packed):
    shifts = jnp.arange(32, dtype=jnp.int32)
    bit_grid = jnp.bitwise_and(jnp.right_shift(packed[:, None, :], shifts[None, :, None]), 1)
    return bit_grid.reshape(packed.shape[0] * 32, packed.shape[1]).astype(jnp.float32)


def reference(light_bits, hub_bits, hub_ids):
    total = light_bits.shape[1]
    vertex_ids = jnp.arange(total, dtype=jnp.int32)
    is_hub = jnp.any(vertex_ids[:, None] == hub_ids[None, :], axis=1)
    light = jnp.where(is_hub, 0.0, 1.0).astype(jnp.float32)
    adjacency = unpack(light_bits) * light[:, None] * light[None, :]
    two_paths = jnp.dot(adjacency, adjacency, precision=lax.Precision.HIGHEST, preferred_element_type=jnp.float32)
    light_tri = 0.5 * jnp.sum(adjacency * two_paths, axis=1)
    hub_rows = unpack(hub_bits) * light[None, :]
    reach_hub = jnp.dot(hub_rows, adjacency, precision=lax.Precision.HIGHEST, preferred_element_type=jnp.float32)
    intersect = hub_rows * reach_hub
    hub_tri = 0.5 * jnp.sum(intersect, axis=1)
    hub_deg = jnp.sum(hub_rows, axis=1)
    owners = (vertex_ids[:, None] == hub_ids[None, :]).astype(jnp.float32)
    triangles = light_tri + jnp.sum(intersect, axis=0) + jnp.sum(owners * hub_tri[None, :], axis=1)
    degrees = jnp.sum(adjacency, axis=1) + jnp.sum(hub_rows, axis=0) + jnp.sum(owners * hub_deg[None, :], axis=1)
    return triangles / (1.0 + degrees)
```

```python
import functools
import math

import jax
import jax.numpy as jnp
from jax import lax
from jax.experimental import pallas as pl
from jax.experimental.pallas import tpu as pltpu
from jax.sharding import PartitionSpec as P

LANES = 128
MESH = pl.DeviceIdType.MESH


def spread(row, value, other=0.0):
    masks = jnp.left_shift(jnp.int32(1), lax.broadcasted_iota(jnp.int32, (32, row.shape[1]), 0))
    return jnp.where((jnp.broadcast_to(row, masks.shape) & masks) != 0, value, other)


def kernel(
    R, C, G,
    light_hbm, hub_hbm, ids_hbm, out_ref,
    ids_ref, rowbuf, colbuf, hubbuf, keep, hubcol, abuf, bbuf, acc, wsum, outbox, inbox, flags,
    local_sem, row_send, row_recv, col_send, col_recv, hub_send, hub_recv, msg_send, msg_recv,
):
    r, c, g = lax.axis_index("rows"), lax.axis_index("cols"), lax.axis_index("hub")
    _, bw, bc = rowbuf.shape
    hw = hubbuf.shape[1]
    pc = bc // G
    q = C // R
    rows = 32 * bw
    wq = bw // q
    nh = 32 * hw * G
    per = rows // C
    me = g * C + c

    own = [
        pltpu.make_async_copy(light_hbm, rowbuf.at[c], local_sem.at[0]),
        pltpu.make_async_copy(hub_hbm, hubbuf.at[me], local_sem.at[1]),
        pltpu.make_async_copy(light_hbm, colbuf.at[r], local_sem.at[2]),
        pltpu.make_async_copy(ids_hbm, ids_ref, local_sem.at[3]),
    ]
    for copy in own:
        copy.start()

    def group_peer(d):
        slot = lax.rem(me + d, G * C)
        return slot, (r, lax.rem(slot, C), slot // C)

    def col_peer(d):
        slot = lax.rem(r + d, R)
        return slot, (slot, c, g)

    barrier = pltpu.get_barrier_semaphore()
    for d in range(1, G * C):
        pl.semaphore_signal(barrier, inc=1, device_id=group_peer(d)[1], device_id_type=MESH)
    for d in range(1, R):
        pl.semaphore_signal(barrier, inc=1, device_id=col_peer(d)[1], device_id_type=MESH)

    for copy in own:
        copy.wait()
    pl.semaphore_wait(barrier, G * C - 1 + R - 1)

    half = C // 2
    home = c // q == r
    inner = jnp.logical_and(4 * c >= C, 4 * c < 3 * C)

    def hub_copy(dj, d):
        return pltpu.make_async_remote_copy(
            src_ref=hubbuf.at[me], dst_ref=hubbuf.at[me], send_sem=hub_send.at[dj * C + d],
            recv_sem=hub_recv.at[me], device_id_type=MESH,
            device_id=(r, lax.rem(c + C - d, C), lax.rem(g + G - dj, G)))

    hub_offsets = [(dj, d) for d in range(C - 1, -1, -1) for dj in range(G) if dj or d]

    def hub_moves(act):
        for dj, d in hub_offsets:
            if d <= half:
                act(dj, d)
            else:
                pl.when(home)(functools.partial(act, dj, d))

    hub_moves(lambda dj, d: hub_copy(dj, d).start())
    sends = []
    for d in range(half, 0, -1):
        sends.append(pltpu.make_async_remote_copy(
            src_ref=rowbuf.at[c], dst_ref=rowbuf.at[c], send_sem=row_send.at[d], recv_sem=row_recv.at[c],
            device_id=(r, lax.rem(c + C - d, C), g), device_id_type=MESH))
    for d in range(1, R):
        sends.append(pltpu.make_async_remote_copy(
            src_ref=colbuf.at[r], dst_ref=colbuf.at[r], send_sem=col_send.at[d], recv_sem=col_recv.at[r],
            device_id=col_peer(d)[1], device_id_type=MESH))
    pl.when(jnp.logical_not(inner))(sends[0].start)
    for copy in sends[1:]:
        copy.start()

    for h in range(nh // LANES):
        hubcol[h * LANES:(h + 1) * LANES, :] = jnp.transpose(
            jnp.broadcast_to(ids_ref[h:h + 1, :], (LANES, LANES)))

    def hub_hits(base):
        return hubcol[...] == base + lax.broadcasted_iota(jnp.int32, (nh, LANES), 1)

    def light_lanes(t, carry):
        hit = jnp.max(jnp.where(hub_hits(t * LANES), 1, 0), axis=0, keepdims=True)
        keep[pl.ds(t, 1), :] = hit - 1
        return carry

    tiles = bc // LANES
    lax.fori_loop(0, C * tiles, light_lanes, 0)

    def keep_of(block):
        return jnp.concatenate([keep[pl.ds(block * tiles + t, 1), :] for t in range(tiles)], axis=1)

    part = pl.ds(pl.multiple_of(g * pc, LANES), pc)
    first = (g == 0).astype(jnp.float32)
    ones = jnp.full((bc, LANES), 1.0, jnp.float32)

    def load(d):
        ck = lax.rem(c + d, C)
        rk = ck // q
        base = d * bc + (nh if d else 0)
        weight = 1.0 if d == 0 else 2.0
        word0 = lax.rem(ck, q) * wq
        for w in range(wq):
            at = base + 32 * w
            bbuf[at:at + 32, :pc] = spread(colbuf[rk, pl.ds(word0 + w, 1), part], weight).astype(jnp.bfloat16)
        if d == 0:
            bbuf[base:base + bc, pc:] = (ones * first).astype(jnp.bfloat16)
        mask = keep_of(ck)
        for w in range(bw):
            abuf[32 * w:32 * w + 32, base:base + bc] = spread(
                rowbuf[ck, w:w + 1, :] & mask, 1.0).astype(jnp.bfloat16)
        for j in range(G):
            for w in range(hw):
                at = rows + 32 * (j * hw + w)
                abuf[at:at + 32, base:base + bc] = spread(
                    hubbuf[j * C + ck, w:w + 1, :] & mask, 1.0).astype(jnp.bfloat16)

    for d in range(1, R):
        slot = col_peer(d)[0]
        pltpu.make_async_copy(colbuf.at[slot], colbuf.at[slot], col_recv.at[slot]).wait()
    load(0)

    def hub_wait(slot):
        pltpu.make_async_copy(hubbuf.at[slot], hubbuf.at[slot], hub_recv.at[slot]).wait()

    for dj, d in hub_offsets:
        ck = lax.rem(c + d, C)
        wait = functools.partial(hub_wait, lax.rem(g + dj, G) * C + ck)
        if d <= half:
            wait()
        else:
            pl.when(ck // q == r)(wait)

    once = first * (c == 0).astype(jnp.float32)
    for j in range(G):
        for w in range(hw):
            at = bc + 32 * (j * hw + w)
            bbuf[at:at + 32, :pc] = spread(hubbuf[j * C + c, w:w + 1, part], 2.0).astype(jnp.bfloat16)
    bbuf[bc:bc + nh, pc:] = jnp.broadcast_to(once, (nh, LANES)).astype(jnp.bfloat16)
    abuf[rows:, bc:bc + nh] = jnp.zeros((nh, nh), jnp.bfloat16)
    for j in range(G):
        for k in range(q):
            bits = jnp.concatenate(
                [spread(hubbuf[j * C + r * q + k, w:w + 1, :], 1.0) for w in range(hw)], axis=0)
            lanes = slice(bc + 32 * hw * j, bc + 32 * hw * (j + 1))
            abuf[k * bc:(k + 1) * bc, lanes] = jnp.transpose(bits).astype(jnp.bfloat16)
    done = bc + nh
    acc[...] = jnp.dot(abuf[:, :done], bbuf[:done, :], preferred_element_type=jnp.float32)

    def settle(to, d):
        hits = hub_hits(r * rows + to * per)
        light = 1.0 - jnp.sum(jnp.where(hits, 1.0, 0.0), axis=0, keepdims=True)
        start = pl.multiple_of(to * per, 8)
        own_sum = jnp.transpose(acc[pl.ds(start, LANES), pc:])[:1, :]
        outbox[d, 1:2, :] = light * own_sum + jnp.sum(
            jnp.where(hits, acc[rows:, pc:], 0.0), axis=0, keepdims=True)
        flags[d] = light

    for d in range(G * C):
        settle(lax.rem(group_peer(d)[0], C), d)

    def meet(d):
        ck = lax.rem(c + d, C)
        pltpu.make_async_copy(rowbuf.at[ck], rowbuf.at[ck], row_recv.at[ck]).wait()
        load(d)

    def add(begin, end):
        acc[:, :pc] += jnp.dot(abuf[:, begin:end], bbuf[begin:end, :pc], preferred_element_type=jnp.float32)

    for d in range(1, half):
        meet(d)
        if d % 2 == 0 or d == half - 1:
            add(done, (d + 1) * bc + nh)
            done = (d + 1) * bc + nh

    @pl.when(inner)
    def _():
        meet(half)
        add(done, (half + 1) * bc + nh)

    mask = jnp.concatenate(
        [keep[pl.ds(c * tiles + g * (pc // LANES) + t, 1), :] for t in range(pc // LANES)], axis=1)

    def close(row, at):
        hit = spread(row & mask, acc[at:at + 32, :pc])
        wsum[at:at + 32, :] = functools.reduce(
            jnp.add, [hit[:, t * LANES:(t + 1) * LANES] for t in range(pc // LANES)])

    for w in range(bw):
        close(rowbuf[c, w:w + 1, part], 32 * w)
    for j in range(G):
        for w in range(hw):
            close(hubbuf[j * C + c, w:w + 1, part], rows + 32 * (j * hw + w))

    hub_tri = jnp.sum(wsum[rows:, :], axis=1, keepdims=True)

    def partial(to, d):
        hits = hub_hits(r * rows + to * per)
        start = pl.multiple_of(to * per, 8)
        own_sum = jnp.sum(jnp.transpose(wsum[pl.ds(start, LANES), :]), axis=0, keepdims=True)
        return flags[d] * own_sum + jnp.sum(jnp.where(hits, hub_tri, 0.0), axis=0, keepdims=True)

    posts = []
    for d in sorted(range(1, G * C), key=lambda d: abs(2 * d - G * C)):
        slot, peer = group_peer(d)
        outbox[d, 0:1, :] = partial(lax.rem(slot, C), d)
        post = pltpu.make_async_remote_copy(
            src_ref=outbox.at[d], dst_ref=inbox.at[me], send_sem=msg_send.at[d], recv_sem=msg_recv.at[me],
            device_id=peer, device_id_type=MESH)
        post.start()
        posts.append(post)

    tri = partial(c, 0)
    deg = outbox[0, 1:2, :]
    for d in range(1, G * C):
        slot, _ = group_peer(d)
        pltpu.make_async_copy(inbox.at[slot], inbox.at[slot], msg_recv.at[slot]).wait()
        tri = tri + inbox[slot, 0:1, :]
        deg = deg + inbox[slot, 1:2, :]
    out_ref[...] = (0.5 * tri / (1.0 + deg))[:, :per]
    hub_moves(lambda dj, d: hub_copy(dj, d).wait_send())
    pl.when(jnp.logical_not(inner))(sends[0].wait_send)
    for copy in sends[1:] + posts:
        copy.wait_send()


def body(light_bits, hub_bits, hub_ids):
    R, C, G = lax.axis_size("rows"), lax.axis_size("cols"), lax.axis_size("hub")
    bw, bc = light_bits.shape
    hw = hub_bits.shape[0]
    nh = hub_ids.shape[0]
    rows, pc = 32 * bw, bc // G
    per = rows // C
    depth = (C // 2 + 1) * bc + nh
    dma = pltpu.SemaphoreType.DMA
    hbm = pl.BlockSpec(memory_space=pltpu.HBM)
    buffers = [
        ((nh // LANES, LANES), jnp.int32),
        ((C, bw, bc), jnp.int32),
        ((R, bw, bc), jnp.int32),
        ((G * C, hw, bc), jnp.int32),
        ((C * bc // LANES, LANES), jnp.int32),
        ((nh, LANES), jnp.int32),
        ((rows + nh, depth), jnp.bfloat16),
        ((depth, pc + LANES), jnp.bfloat16),
        ((rows + nh, pc + LANES), jnp.float32),
        ((rows + nh, LANES), jnp.float32),
        ((G * C, 2, LANES), jnp.float32),
        ((G * C, 2, LANES), jnp.float32),
        ((G * C, 1, LANES), jnp.float32),
    ]
    held = sum(math.prod(shape) * jnp.dtype(dtype).itemsize for shape, dtype in buffers)
    out = pl.pallas_call(
        functools.partial(kernel, R, C, G),
        out_shape=jax.ShapeDtypeStruct((1, per), jnp.float32),
        in_specs=[hbm, hbm, hbm],
        out_specs=pl.BlockSpec(memory_space=pltpu.VMEM),
        scratch_shapes=[pltpu.VMEM(shape, dtype) for shape, dtype in buffers] + [
            dma((4,)), dma((C,)), dma((C,)), dma((R,)), dma((R,)),
            dma((G * C,)), dma((G * C,)), dma((G * C,)), dma((G * C,)),
        ],
        compiler_params=pltpu.CompilerParams(
            collective_id=0, has_side_effects=True, vmem_limit_bytes=held + 12 * 1024 * 1024),
    )(*(pltpu.with_memory_space_constraint(x, pltpu.HBM)
        for x in (light_bits, hub_bits, hub_ids.reshape(nh // LANES, LANES))))
    return out.reshape(per)


def solution(mesh):
    return jax.shard_map(
        body,
        mesh=mesh,
        in_specs=(P("rows", "cols"), P("hub", "cols"), P()),
        out_specs=P(("rows", "cols")),
        check_vma=False,
    )
```

```python
import functools
import math

import jax
import jax.numpy as jnp
from jax import lax
from jax.experimental import pallas as pl
from jax.experimental.pallas import tpu as pltpu
from jax.sharding import PartitionSpec as P

LANES = 128
MESH = pl.DeviceIdType.MESH


def spread(row, value, other=0.0):
    masks = jnp.left_shift(jnp.int32(1), lax.broadcasted_iota(jnp.int32, (32, row.shape[1]), 0))
    return jnp.where((jnp.broadcast_to(row, masks.shape) & masks) != 0, value, other)


def piece(bw, wq, q):
    starts = [x * wq // 8 * 8 for x in range(q)]
    size = max(-(-(x + 1) * wq // 8) * 8 - starts[x] for x in range(q))
    if max(starts) + size > bw:
        return 0, bw
    return 8, size


def kernel(
    R, C, G,
    light_hbm, hub_hbm, ids_hbm, out_ref,
    ids_ref, rowbuf, colbuf, hubbuf, keep, hubcol, abuf, bbuf, home, degs, wsum, outbox, inbox, flags,
    local_sem, row_send, row_recv, col_send, col_recv, hub_send, hub_recv, msg_send, msg_recv,
):
    r, c, g = lax.axis_index("rows"), lax.axis_index("cols"), lax.axis_index("hub")
    _, bw, bc = rowbuf.shape
    hw = hubbuf.shape[1]
    pc = bc // G
    q = C // R
    z, x = c // q, c % q
    rows = 32 * bw
    wq = bw // q
    ng = 32 * hw
    nh = ng * G
    per = rows // C
    me = g * C + c
    unit, size = piece(bw, wq, q)

    def begin(x):
        return x * wq // unit * unit if unit else 0 * x

    own = [
        pltpu.make_async_copy(light_hbm, rowbuf.at[c], local_sem.at[0]),
        pltpu.make_async_copy(hub_hbm, hubbuf.at[me], local_sem.at[1]),
        pltpu.make_async_copy(ids_hbm, ids_ref, local_sem.at[2]),
    ]
    for copy in own:
        copy.start()

    def at(plane, dx, dg=0):
        return (r, plane * q + (x + dx) % q, (g + dg) % G)

    barrier = pltpu.get_barrier_semaphore()

    def greet(device):
        pl.semaphore_signal(barrier, inc=1, device_id=device, device_id_type=MESH)

    for dz in range(R):
        @pl.when(z + dz < R)
        def _():
            for dx in range(q):
                for dg in range(G):
                    if dz or dx or dg:
                        greet(at(z + dz, dx, dg))
    for dr in range(1, R):
        @pl.when((r + dr) % R >= z)
        def _():
            for dx in range(q):
                greet(((r + dr) % R, z * q + dx, g))

    def row_copy(dz, dx):
        return pltpu.make_async_remote_copy(
            src_ref=rowbuf.at[c], dst_ref=rowbuf.at[c], send_sem=row_send.at[dz, dx], recv_sem=row_recv.at[c],
            device_id=at(z - dz, dx), device_id_type=MESH)

    def hub_copy(dz, dx, dg):
        return pltpu.make_async_remote_copy(
            src_ref=hubbuf.at[me], dst_ref=hubbuf.at[me], send_sem=hub_send.at[dz, dx, dg],
            recv_sem=hub_recv.at[me], device_id=at(z - dz, dx, dg), device_id_type=MESH)

    def col_copy(dr, tx):
        return pltpu.make_async_remote_copy(
            src_ref=rowbuf.at[c, pl.ds(begin(tx), size), :], dst_ref=colbuf.at[r, x],
            send_sem=col_send.at[dr, tx], recv_sem=col_recv.at[r, x],
            device_id=((r + dr) % R, z * q + tx, g), device_id_type=MESH)

    def moves(act):
        for dz in range(R - 1, -1, -1):
            @pl.when(z >= dz)
            def _():
                for dx in range(q):
                    for dg in range(G):
                        if dz or dx or dg:
                            act(hub_copy(dz, dx, dg))
                if dz:
                    act(row_copy(dz, 0))
                else:
                    for dx in range(1, q):
                        act(row_copy(0, dx))

        @pl.when(r >= z)
        def _():
            for dr in range(1, R):
                for tx in range(q):
                    act(col_copy(dr, tx))

    for copy in own:
        copy.wait()
    pl.semaphore_wait(barrier, (z + 1) * q * G - 1 + jnp.where(r >= z, (R - 1) * q, 0))
    moves(lambda copy: copy.start())

    for h in range(nh // LANES):
        hubcol[h * LANES:(h + 1) * LANES, :] = jnp.transpose(
            jnp.broadcast_to(ids_ref[h:h + 1, :], (LANES, LANES)))

    def hub_hits(base):
        return hubcol[...] == base + lax.broadcasted_iota(jnp.int32, (nh, LANES), 1)

    def light_lanes(t, carry):
        hit = jnp.max(jnp.where(hub_hits(t * LANES), 1, 0), axis=0, keepdims=True)
        keep[pl.ds(t, 1), :] = hit - 1
        return carry

    tiles = bc // LANES
    lax.fori_loop(0, C * tiles, light_lanes, 0)

    def keep_of(block, first=0, count=tiles):
        return jnp.concatenate([keep[pl.ds(block * tiles + first + t, 1), :] for t in range(count)], axis=1)

    part = pl.ds(pl.multiple_of(g * pc, LANES), pc)
    once = (g == 0).astype(jnp.float32)
    wide = q * pc + ng

    def wait_row(k):
        pltpu.make_async_copy(rowbuf.at[k], rowbuf.at[k], row_recv.at[k]).wait()

    def wait_hub(slot):
        pltpu.make_async_copy(hubbuf.at[slot], hubbuf.at[slot], hub_recv.at[slot]).wait()

    def wait_col(plane, tx):
        pltpu.make_async_copy(colbuf.at[plane, tx], colbuf.at[plane, tx], col_recv.at[plane, tx]).wait()

    def load_a(k):
        mask = keep_of(k)
        for w in range(bw):
            abuf[32 * w:32 * w + 32, :] = spread(rowbuf[k, w:w + 1, :] & mask, 1.0).astype(jnp.bfloat16)
        for j in range(G):
            for w in range(hw):
                lo = rows + 32 * (j * hw + w)
                abuf[lo:lo + 32, :] = spread(hubbuf[j * C + k, w:w + 1, :] & mask, 1.0).astype(jnp.bfloat16)

    def hub_rows(block, value):
        return jnp.transpose(jnp.concatenate(
            [spread(hubbuf[g * C + block, w:w + 1, :], value) for w in range(hw)], axis=0))

    def load_b(plane, weight):
        for tx in range(q):
            for w in range(wq):
                bits = colbuf[plane, tx, pl.ds(x * wq - begin(x) + w, 1), part]
                bbuf[32 * w:32 * w + 32, tx * pc:(tx + 1) * pc] = spread(bits, weight).astype(jnp.bfloat16)

        @pl.when(z == 0)
        def _():
            bbuf[:, q * pc:wide] = hub_rows(plane * q + x, 2.0).astype(jnp.bfloat16)

    masks = []

    def close(product, fresh):
        def tail(lo, total):
            wsum[lo:lo + 32, :] = total if fresh else wsum[lo:lo + 32, :] + total

        def hits(words, lo):
            found = []
            for tx in range(q):
                hit = spread(words(tx) & masks[tx], product[lo:lo + 32, tx * pc:(tx + 1) * pc])
                found += [hit[:, t * LANES:(t + 1) * LANES] for t in range(pc // LANES)]
            return functools.reduce(jnp.add, found)

        for w in range(bw):
            lo = 32 * w
            found = hits(lambda tx: rowbuf[z * q + tx, w:w + 1, part], lo)
            for t in range(ng // LANES):
                lanes = slice(t * LANES, (t + 1) * LANES)
                found += home[lo:lo + 32, lanes] * product[lo:lo + 32, q * pc + t * LANES:q * pc + (t + 1) * LANES]
            tail(lo, found)
        for j in range(G):
            for w in range(hw):
                tail(rows + 32 * (j * hw + w),
                     hits(lambda tx: hubbuf[j * C + z * q + tx, w:w + 1, part], rows + 32 * (j * hw + w)))

    load_a(c)
    bbuf[:, wide:] = jnp.broadcast_to(once, (bc, LANES)).astype(jnp.bfloat16)

    @pl.when(z > 0)
    def _():
        bbuf[:, q * pc:wide] = jnp.zeros((bc, ng), jnp.bfloat16)
        home[...] = jnp.zeros((rows, ng), jnp.float32)

    for dx in range(q):
        for dg in range(G):
            if dx or dg:
                wait_hub((g + dg) % G * C + z * q + (x + dx) % q)
        if dx:
            wait_row(z * q + (x + dx) % q)
    for tx in range(q):
        colbuf[r, tx] = rowbuf[z * q + tx, pl.ds(begin(x), size), :]
        masks.append(keep_of(z * q + tx, g * (pc // LANES), pc // LANES))

    @pl.when(r != z)
    def _():
        for tx in range(q):
            wait_col(z, tx)

    for dz in range(1, R):
        @pl.when(z + dz < R)
        def _():
            for dx in range(q):
                for dg in range(G):
                    if dx:
                        wait_hub((g + dg) % G * C + (z + dz) * q + (x + dx) % q)
                    elif dg:
                        wait_hub((g + dg) % G * C + (z + dz) * q + x)
                    else:
                        wait_hub(g * C + (z + dz) * q + x)

    @pl.when(z == 0)
    def _():
        for k in range(q):
            home[k * bc:(k + 1) * bc, :] = hub_rows(r * q + k, 1.0)

    load_b(z, 1.0)
    product = jnp.dot(abuf[...], bbuf[...], preferred_element_type=jnp.float32)
    degs[...] = product[:, wide:]
    close(product, True)

    @pl.when(jnp.logical_and(z == 0, x == 0))
    def _():
        for t in range(ng // LANES):
            degs[:rows, :] += jnp.broadcast_to(
                jnp.sum(home[:, t * LANES:(t + 1) * LANES], axis=1, keepdims=True), (rows, LANES))

    def step(dz, carry):
        plane = z + dz
        k = plane * q + x

        @pl.when(plane != r)
        def _():
            for tx in range(q):
                wait_col(plane, tx)

        wait_row(k)
        load_a(k)
        load_b(plane, 2.0)
        close(jnp.dot(abuf[...], bbuf[:, :wide], preferred_element_type=jnp.float32), False)
        return carry

    lax.fori_loop(1, R - z, step, 0)

    hub_tri = jnp.sum(wsum[rows:, :], axis=1, keepdims=True)
    hub_deg = degs[rows:, :]

    def settle(to, d):
        hits = hub_hits(r * rows + to * per)
        light = 1.0 - jnp.sum(jnp.where(hits, 1.0, 0.0), axis=0, keepdims=True)
        start = pl.multiple_of(to * per, 8)
        tri = jnp.sum(jnp.transpose(wsum[pl.ds(start, LANES), :]), axis=0, keepdims=True)
        deg = jnp.transpose(degs[pl.ds(start, LANES), :])[:1, :]
        outbox[d, 0:1, :] = light * tri + jnp.sum(jnp.where(hits, hub_tri, 0.0), axis=0, keepdims=True)
        outbox[d, 1:2, :] = light * deg + jnp.sum(jnp.where(hits, hub_deg, 0.0), axis=0, keepdims=True)

    posts = []
    for d in range(1, G * C):
        slot = (me + d) % (G * C)
        settle(slot % C, d)
        post = pltpu.make_async_remote_copy(
            src_ref=outbox.at[d], dst_ref=inbox.at[me], send_sem=msg_send.at[d], recv_sem=msg_recv.at[me],
            device_id=(r, slot % C, slot // C), device_id_type=MESH)
        post.start()
        posts.append(post)

    settle(c, 0)
    tri = outbox[0, 0:1, :]
    deg = outbox[0, 1:2, :]
    for d in range(1, G * C):
        slot = (me + d) % (G * C)
        pltpu.make_async_copy(inbox.at[slot], inbox.at[slot], msg_recv.at[slot]).wait()
        tri = tri + inbox[slot, 0:1, :]
        deg = deg + inbox[slot, 1:2, :]
    out_ref[...] = (0.5 * tri / (1.0 + deg))[:, :per]
    moves(lambda copy: copy.wait_send())
    for copy in posts:
        copy.wait_send()


def body(light_bits, hub_bits, hub_ids):
    R, C, G = lax.axis_size("rows"), lax.axis_size("cols"), lax.axis_size("hub")
    bw, bc = light_bits.shape
    hw = hub_bits.shape[0]
    nh = hub_ids.shape[0]
    rows, pc = 32 * bw, bc // G
    per = rows // C
    q = C // R
    wide = q * pc + nh // G
    _, size = piece(bw, bw // q, q)
    dma = pltpu.SemaphoreType.DMA
    hbm = pl.BlockSpec(memory_space=pltpu.HBM)
    buffers = [
        ((nh // LANES, LANES), jnp.int32),
        ((C, bw, bc), jnp.int32),
        ((R, q, size, bc), jnp.int32),
        ((G * C, hw, bc), jnp.int32),
        ((C * bc // LANES, LANES), jnp.int32),
        ((nh, LANES), jnp.int32),
        ((rows + nh, bc), jnp.bfloat16),
        ((bc, wide + LANES), jnp.bfloat16),
        ((rows, nh // G), jnp.float32),
        ((rows + nh, LANES), jnp.float32),
        ((rows + nh, LANES), jnp.float32),
        ((G * C, 2, LANES), jnp.float32),
        ((G * C, 2, LANES), jnp.float32),
        ((G * C, 1, LANES), jnp.float32),
    ]
    held = sum(math.prod(shape) * jnp.dtype(dtype).itemsize for shape, dtype in buffers)
    held += 4 * (rows + nh) * (wide + LANES)
    out = pl.pallas_call(
        functools.partial(kernel, R, C, G),
        out_shape=jax.ShapeDtypeStruct((1, per), jnp.float32),
        in_specs=[hbm, hbm, hbm],
        out_specs=pl.BlockSpec(memory_space=pltpu.VMEM),
        scratch_shapes=[pltpu.VMEM(shape, dtype) for shape, dtype in buffers] + [
            dma((3,)), dma((R, q)), dma((C,)), dma((R, q)), dma((R, q)),
            dma((R, q, G)), dma((G * C,)), dma((G * C,)), dma((G * C,)),
        ],
        compiler_params=pltpu.CompilerParams(
            collective_id=0, has_side_effects=True, vmem_limit_bytes=held + 12 * 1024 * 1024),
    )(*(pltpu.with_memory_space_constraint(x, pltpu.HBM)
        for x in (light_bits, hub_bits, hub_ids.reshape(nh // LANES, LANES))))
    return out.reshape(per)


def solution(mesh):
    return jax.shard_map(
        body,
        mesh=mesh,
        in_specs=(P("rows", "cols"), P("hub", "cols"), P()),
        out_specs=P(("rows", "cols")),
        check_vma=False,
    )
```

```python
import functools
import math

import jax
import jax.numpy as jnp
from jax import lax
from jax.experimental import pallas as pl
from jax.experimental.pallas import tpu as pltpu
from jax.sharding import PartitionSpec as P

LANES = 128
BIT = jnp.float8_e4m3fn
MESH = pl.DeviceIdType.MESH


def spread(row, value, other=0.0):
    masks = jnp.left_shift(jnp.int32(1), lax.broadcasted_iota(jnp.int32, (32, row.shape[1]), 0))
    return jnp.where((jnp.broadcast_to(row, masks.shape) & masks) != 0, value, other)


def piece(bw, wq, q):
    starts = [x * wq // 8 * 8 for x in range(q)]
    size = max(-(-(x + 1) * wq // 8) * 8 - starts[x] for x in range(q))
    if max(starts) + size > bw:
        return 0, bw
    return 8, size


def kernel(
    R, C, G,
    light_hbm, hub_hbm, ids_hbm, out_ref,
    ids_ref, rowbuf, colbuf, hubbuf, keep, hubcol, abuf, bbuf, mask, owner, light, wsum, outbox, inbox,
    local_sem, row_send, row_recv, col_send, col_recv, hub_send, hub_recv, msg_send, msg_recv,
):
    r, c, g = lax.axis_index("rows"), lax.axis_index("cols"), lax.axis_index("hub")
    _, bw, bc = rowbuf.shape
    hw = hubbuf.shape[1]
    pc = bc // G
    q = C // R
    z, x = c // q, c % q
    rows = 32 * bw
    wq = bw // q
    ng = 32 * hw
    nh = ng * G
    per = rows // C
    me = g * C + c
    unit, size = piece(bw, wq, q)

    def begin(x):
        return x * wq // unit * unit if unit else 0 * x

    own = [
        pltpu.make_async_copy(light_hbm, rowbuf.at[c], local_sem.at[0]),
        pltpu.make_async_copy(hub_hbm, hubbuf.at[me], local_sem.at[1]),
        pltpu.make_async_copy(ids_hbm, ids_ref, local_sem.at[2]),
    ]
    for copy in own:
        copy.start()

    def at(plane, dx, dg=0):
        return (r, plane * q + (x + dx) % q, (g + dg) % G)

    barrier = pltpu.get_barrier_semaphore()

    def greet(device):
        pl.semaphore_signal(barrier, inc=1, device_id=device, device_id_type=MESH)

    for dz in range(R):
        @pl.when(z + dz < R)
        def _():
            for dx in range(q):
                for dg in range(G):
                    if dz or dx or dg:
                        greet(at(z + dz, dx, dg))
    for dr in range(1, R):
        @pl.when((r + dr) % R >= z)
        def _():
            for dx in range(q):
                greet(((r + dr) % R, z * q + dx, g))

    def row_copy(dz, dx):
        return pltpu.make_async_remote_copy(
            src_ref=rowbuf.at[c], dst_ref=rowbuf.at[c], send_sem=row_send.at[dz, dx], recv_sem=row_recv.at[c],
            device_id=at(z - dz, dx), device_id_type=MESH)

    def hub_copy(dz, dx, dg):
        return pltpu.make_async_remote_copy(
            src_ref=hubbuf.at[me], dst_ref=hubbuf.at[me], send_sem=hub_send.at[dz, dx, dg],
            recv_sem=hub_recv.at[me], device_id=at(z - dz, dx, dg), device_id_type=MESH)

    def col_copy(dr, tx):
        return pltpu.make_async_remote_copy(
            src_ref=rowbuf.at[c, pl.ds(begin(tx), size), :], dst_ref=colbuf.at[r, x],
            send_sem=col_send.at[dr, tx], recv_sem=col_recv.at[r, x],
            device_id=((r + dr) % R, z * q + tx, g), device_id_type=MESH)

    def moves(act):
        for dz in range(R - 1, -1, -1):
            @pl.when(z >= dz)
            def _():
                for dx in range(q):
                    for dg in range(G):
                        if dz or dx or dg:
                            act(hub_copy(dz, dx, dg))
                if dz:
                    act(row_copy(dz, 0))
                else:
                    for dx in range(1, q):
                        act(row_copy(0, dx))

        @pl.when(r >= z)
        def _():
            for dr in range(1, R):
                for tx in range(q):
                    act(col_copy(dr, tx))

    for copy in own:
        copy.wait()
    pl.semaphore_wait(barrier, (z + 1) * q * G - 1 + jnp.where(r >= z, (R - 1) * q, 0))
    moves(lambda copy: copy.start())

    for h in range(nh // LANES):
        hubcol[h * LANES:(h + 1) * LANES, :] = jnp.transpose(
            jnp.broadcast_to(ids_ref[h:h + 1, :], (LANES, LANES)))

    def hub_hits(base):
        return hubcol[...] == base + lax.broadcasted_iota(jnp.int32, (nh, LANES), 1)

    def light_lanes(t, carry):
        hit = jnp.max(jnp.where(hub_hits(t * LANES), 1, 0), axis=0, keepdims=True)
        keep[pl.ds(t, 1), :] = hit - 1
        return carry

    tiles = bc // LANES
    lax.fori_loop(0, C * tiles, light_lanes, 0)

    def keep_of(block, first=0, count=tiles):
        return jnp.concatenate([keep[pl.ds(block * tiles + first + t, 1), :] for t in range(count)], axis=1)

    part = pl.ds(pl.multiple_of(g * pc, LANES), pc)
    once = (g == 0).astype(jnp.float32)
    wide = q * pc + ng

    def wait_row(k):
        pltpu.make_async_copy(rowbuf.at[k], rowbuf.at[k], row_recv.at[k]).wait()

    def wait_hub(slot):
        pltpu.make_async_copy(hubbuf.at[slot], hubbuf.at[slot], hub_recv.at[slot]).wait()

    def wait_col(plane, tx):
        pltpu.make_async_copy(colbuf.at[plane, tx], colbuf.at[plane, tx], col_recv.at[plane, tx]).wait()

    def load_light(k):
        kept = keep_of(k)
        for w in range(bw):
            abuf[32 * w:32 * w + 32, :] = spread(rowbuf[k, w:w + 1, :] & kept, 1.0).astype(BIT)

    def load_hubs(k):
        kept = keep_of(k)
        for j in range(G):
            for w in range(hw):
                lo = rows + 32 * (j * hw + w)
                abuf[lo:lo + 32, :] = spread(hubbuf[j * C + k, w:w + 1, :] & kept, 1.0).astype(BIT)

    def hub_rows(block, value):
        return jnp.transpose(jnp.concatenate(
            [spread(hubbuf[g * C + block, w:w + 1, :], value) for w in range(hw)], axis=0))

    def load_side(plane):
        @pl.when(z == 0)
        def _():
            bbuf[:, q * pc:] = hub_rows(plane * q + x, 2.0).astype(BIT)

    def load_b(plane, weight):
        for tx in range(q):
            for w in range(wq):
                bits = colbuf[plane, tx, pl.ds(x * wq - begin(x) + w, 1), part]
                bbuf[32 * w:32 * w + 32, tx * pc:(tx + 1) * pc] = spread(bits, weight).astype(BIT)

    def close(product, fresh):
        for lo in range(0, rows + nh, 32):
            found = functools.reduce(jnp.add, [
                mask[lo:lo + 32, at:at + LANES] * product[lo:lo + 32, at:at + LANES]
                for at in range(0, wide if lo < rows else q * pc, LANES)])
            wsum[lo:lo + 32, :] = found if fresh else wsum[lo:lo + 32, :] + found

    load_light(c)
    for t in range(rows // LANES):
        lanes = slice(t * LANES, (t + 1) * LANES)
        hits = jnp.where(hub_hits(r * rows + t * LANES), 1.0, 0.0)
        owner[:, lanes] = hits
        light[:, lanes] = 1.0 - jnp.sum(hits, axis=0, keepdims=True)

    @pl.when(z > 0)
    def _():
        bbuf[:, q * pc:] = jnp.zeros((bc, ng), BIT)
        mask[:rows, q * pc:] = jnp.zeros((rows, ng), jnp.float32)

    for dx in range(q):
        for dg in range(G):
            if dx or dg:
                wait_hub((g + dg) % G * C + z * q + (x + dx) % q)
        if dx:
            wait_row(z * q + (x + dx) % q)
    load_hubs(c)
    for tx in range(q):
        colbuf[r, tx] = rowbuf[z * q + tx, pl.ds(begin(x), size), :]
        kept = keep_of(z * q + tx, g * (pc // LANES), pc // LANES)
        lanes = slice(tx * pc, (tx + 1) * pc)
        for w in range(bw):
            mask[32 * w:32 * w + 32, lanes] = spread(rowbuf[z * q + tx, w:w + 1, part] & kept, 1.0)
        for j in range(G):
            for w in range(hw):
                lo = rows + 32 * (j * hw + w)
                mask[lo:lo + 32, lanes] = spread(hubbuf[j * C + z * q + tx, w:w + 1, part] & kept, 1.0)

    def over_lanes(row):
        return functools.reduce(jnp.add, [row[:, t * LANES:(t + 1) * LANES] for t in range(tiles)])

    kept = keep_of(c)
    hub_deg = jnp.sum(jnp.concatenate([
        over_lanes(spread(hubbuf[j * C + c, w:w + 1, :] & kept, 1.0)) for j in range(G) for w in range(hw)],
        axis=0), axis=1, keepdims=True) * once

    def turn(matrix):
        ones = jnp.ones((8, matrix.shape[1]), matrix.dtype)
        return lax.dot_general(
            ones, matrix, (((1,), (1,)), ((), ())), preferred_element_type=jnp.float32)[:1, :]

    def owned(row, column):
        return light[...] * row + jnp.sum(owner[...] * column, axis=0, keepdims=True)

    deg_row = owned(turn(abuf[:rows, :]) * once, hub_deg)

    def post(row, value):
        for slot in range(G * C):
            to = slot % C
            outbox[slot, row:row + 1, :per] = value[:, to * per:(to + 1) * per]

    post(1, deg_row)

    @pl.when(r != z)
    def _():
        for tx in range(q):
            wait_col(z, tx)

    for dz in range(1, R):
        @pl.when(z + dz < R)
        def _():
            for dx in range(q):
                for dg in range(G):
                    wait_hub((g + dg) % G * C + (z + dz) * q + (x + dx) % q)

    @pl.when(z == 0)
    def _():
        for k in range(q):
            mask[k * bc:(k + 1) * bc, q * pc:] = hub_rows(r * q + k, 1.0)

    @pl.when(jnp.logical_and(z == 0, x == 0))
    def _():
        extra = light[...] * jnp.concatenate([
            jnp.sum(functools.reduce(jnp.add, [
                spread(hubbuf[g * C + r * q + k, w:w + 1, :], 1.0) for w in range(hw)]), axis=0, keepdims=True)
            for k in range(q)], axis=1)
        post(1, deg_row + extra)

    load_side(z)
    load_b(z, 1.0)
    close(jnp.dot(abuf[...], bbuf[...], preferred_element_type=jnp.float32), True)

    def step(dz, carry):
        plane = z + dz
        k = plane * q + x

        @pl.when(plane != r)
        def _():
            for tx in range(q):
                wait_col(plane, tx)

        load_side(plane)
        wait_row(k)
        load_b(plane, 2.0)
        load_hubs(k)
        load_light(k)
        close(jnp.dot(abuf[...], bbuf[...], preferred_element_type=jnp.float32), False)
        return carry

    lax.fori_loop(1, R - z, step, 0)

    hub_tri = jnp.sum(wsum[rows:, :], axis=1, keepdims=True)
    rest = wsum[:rows, :]
    tri_row = jnp.zeros((1, rows), jnp.float32)
    for _ in range(3):
        upper = rest.astype(jnp.bfloat16)
        tri_row = tri_row + turn(upper)
        rest = rest - upper.astype(jnp.float32)
    post(0, owned(tri_row, hub_tri))

    def message(slot):
        return pltpu.make_async_remote_copy(
            src_ref=outbox.at[slot], dst_ref=inbox.at[me], send_sem=msg_send.at[slot], recv_sem=msg_recv.at[me],
            device_id=(r, slot % C, slot // C), device_id_type=MESH)

    def messages(act):
        for slot in range(G * C):
            @pl.when(slot != me)
            def _():
                act(message(slot))

    messages(lambda copy: copy.start())
    tri = outbox[me, 0:1, :]
    deg = outbox[me, 1:2, :]
    for d in range(1, G * C):
        slot = (me + d) % (G * C)
        pltpu.make_async_copy(inbox.at[slot], inbox.at[slot], msg_recv.at[slot]).wait()
        tri = tri + inbox[slot, 0:1, :]
        deg = deg + inbox[slot, 1:2, :]
    out_ref[...] = (0.5 * tri / (1.0 + deg))[:, :per]
    moves(lambda copy: copy.wait_send())
    messages(lambda copy: copy.wait_send())


def body(light_bits, hub_bits, hub_ids):
    R, C, G = lax.axis_size("rows"), lax.axis_size("cols"), lax.axis_size("hub")
    bw, bc = light_bits.shape
    hw = hub_bits.shape[0]
    nh = hub_ids.shape[0]
    rows, pc = 32 * bw, bc // G
    per = rows // C
    q = C // R
    wide = q * pc + nh // G
    _, size = piece(bw, bw // q, q)
    dma = pltpu.SemaphoreType.DMA
    hbm = pl.BlockSpec(memory_space=pltpu.HBM)
    buffers = [
        ((nh // LANES, LANES), jnp.int32),
        ((C, bw, bc), jnp.int32),
        ((R, q, size, bc), jnp.int32),
        ((G * C, hw, bc), jnp.int32),
        ((C * bc // LANES, LANES), jnp.int32),
        ((nh, LANES), jnp.int32),
        ((rows + nh, bc), BIT),
        ((bc, wide), BIT),
        ((rows + nh, wide), jnp.float32),
        ((nh, rows), jnp.float32),
        ((1, rows), jnp.float32),
        ((rows + nh, LANES), jnp.float32),
        ((G * C, 2, LANES), jnp.float32),
        ((G * C, 2, LANES), jnp.float32),
    ]
    held = sum(math.prod(shape) * jnp.dtype(dtype).itemsize for shape, dtype in buffers)
    held += 4 * (rows + nh) * wide
    out = pl.pallas_call(
        functools.partial(kernel, R, C, G),
        out_shape=jax.ShapeDtypeStruct((1, per), jnp.float32),
        in_specs=[hbm, hbm, hbm],
        out_specs=pl.BlockSpec(memory_space=pltpu.VMEM),
        scratch_shapes=[pltpu.VMEM(shape, dtype) for shape, dtype in buffers] + [
            dma((3,)), dma((R, q)), dma((C,)), dma((R, q)), dma((R, q)),
            dma((R, q, G)), dma((G * C,)), dma((G * C,)), dma((G * C,)),
        ],
        compiler_params=pltpu.CompilerParams(
            collective_id=0, has_side_effects=True, vmem_limit_bytes=held + 12 * 1024 * 1024),
    )(*(pltpu.with_memory_space_constraint(x, pltpu.HBM)
        for x in (light_bits, hub_bits, hub_ids.reshape(nh // LANES, LANES))))
    return out.reshape(per)


def solution(mesh):
    return jax.shard_map(
        body,
        mesh=mesh,
        in_specs=(P("rows", "cols"), P("hub", "cols"), P()),
        out_specs=P(("rows", "cols")),
        check_vma=False,
    )
```

```python
import functools
import math

import jax
import jax.numpy as jnp
from jax import lax
from jax.experimental import pallas as pl
from jax.experimental.pallas import tpu as pltpu
from jax.sharding import PartitionSpec as P

LANES = 128
BIT = jnp.float8_e4m3fn
MESH = pl.DeviceIdType.MESH


def spread(row, value, other=0.0):
    masks = jnp.left_shift(jnp.int32(1), lax.broadcasted_iota(jnp.int32, (32, row.shape[1]), 0))
    return jnp.where((jnp.broadcast_to(row, masks.shape) & masks) != 0, value, other)


def pieces(wq, x):
    cuts = [x * wq] + [t for t in range(8, (x + 1) * wq, 8) if t > x * wq] + [(x + 1) * wq]
    parts = []
    for lo, hi in zip(cuts, cuts[1:]):
        if parts and lo % 8 == 0 and hi % 8 == 0 and parts[-1][0] % 8 == 0 and sum(parts[-1]) == lo:
            parts[-1] = (parts[-1][0], hi - parts[-1][0])
        else:
            parts.append((lo, hi - lo))
    return parts


def shape_of(wq, q):
    size = max(-(-(x + 1) * wq // 8) * 8 - x * wq // 8 * 8 for x in range(q))
    return size, max(len(pieces(wq, x)) for x in range(q))


def kernel(
    R, C, G,
    light_hbm, hub_hbm, ids_hbm, out_ref,
    ids_ref, rowbuf, colbuf, hubbuf, keep, hubcol, abuf, bbuf, home, side, owner, light, product, wsum, outbox, inbox,
    local_sem, row_send, row_recv, col_send, col_recv, hub_send, hub_recv, msg_send, msg_recv, seen,
):
    r, c, g = lax.axis_index("rows"), lax.axis_index("cols"), lax.axis_index("hub")
    _, bw, bc = rowbuf.shape
    hw = hubbuf.shape[1]
    pc = bc // G
    q = C // R
    z, x = c // q, c % q
    rows = 32 * bw
    wq = bw // q
    ng = 32 * hw
    nh = ng * G
    per = rows // C
    me = g * C + c

    own = [
        pltpu.make_async_copy(light_hbm, rowbuf.at[c], local_sem.at[0]),
        pltpu.make_async_copy(hub_hbm, hubbuf.at[me], local_sem.at[1]),
        pltpu.make_async_copy(ids_hbm, ids_ref, local_sem.at[2]),
    ]
    for copy in own:
        copy.start()

    def at(plane, dx, dg=0):
        return (r, plane * q + (x + dx) % q, (g + dg) % G)

    barrier = pltpu.get_barrier_semaphore()

    def greet(device):
        pl.semaphore_signal(barrier, inc=1, device_id=device, device_id_type=MESH)

    for dz in range(R):
        @pl.when(z + dz < R)
        def _():
            for dx in range(q):
                for dg in range(G):
                    if dz or dx or dg:
                        greet(at(z + dz, dx, dg))
    for dr in range(1, R):
        @pl.when((r + dr) % R >= z)
        def _():
            for dx in range(q):
                greet(((r + dr) % R, z * q + dx, g))

    def row_copy(dz, dx):
        return pltpu.make_async_remote_copy(
            src_ref=rowbuf.at[c], dst_ref=rowbuf.at[c], send_sem=row_send.at[dz, dx], recv_sem=row_recv.at[c],
            device_id=at(z - dz, dx), device_id_type=MESH)

    def hub_copy(dz, dx, dg):
        return pltpu.make_async_remote_copy(
            src_ref=hubbuf.at[me], dst_ref=hubbuf.at[me], send_sem=hub_send.at[dz, dx, dg],
            recv_sem=hub_recv.at[me], device_id=at(z - dz, dx, dg), device_id_type=MESH)

    def homing(dx):
        return pltpu.make_async_remote_copy(
            src_ref=hubbuf.at[me], dst_ref=hubbuf.at[me], send_sem=hub_send.at[R, dx, 0],
            recv_sem=hub_recv.at[me], device_id=at(0, dx), device_id_type=MESH)

    def col_copies(to, tx):
        base = tx * wq // 8 * 8
        return [
            pltpu.make_async_remote_copy(
                src_ref=rowbuf.at[c, pl.ds(lo, size), :], dst_ref=colbuf.at[r, x, pl.ds(lo - base, size), :],
                send_sem=col_send.at[to, tx, n], recv_sem=col_recv.at[r, x, n],
                device_id=(to, z * q + tx, g), device_id_type=MESH)
            for n, (lo, size) in enumerate(pieces(wq, tx))]

    def moves(act):
        @pl.when(jnp.logical_and(z == r, z > 0))
        def _():
            for dx in range(1, q):
                act(homing(dx))

        for dz in range(R - 1, -1, -1):
            @pl.when(z >= dz)
            def _():
                for dx in range(q if dz == 0 else 1):
                    for dg in range(G):
                        if dz or dx or dg:
                            act(hub_copy(dz, dx, dg))
                if dz:
                    act(row_copy(dz, 0))
                else:
                    for dx in range(1, q):
                        act(row_copy(0, dx))

        @pl.when(r >= z)
        def _():
            for to in range(R):
                @pl.when(r != to)
                def _():
                    for tx in range(q):
                        for copy in col_copies(to, tx):
                            act(copy)

    for copy in own:
        copy.wait()
    pl.semaphore_wait(barrier, (z + 1) * q * G - 1 + jnp.where(r >= z, (R - 1) * q, 0))
    moves(lambda copy: copy.start())
    for dz in range(1, R):
        for dx in range(1, q):
            for dg in range(G):
                homed = jnp.logical_and(z == r, z == dz) if dg == 0 else False

                @pl.when(jnp.logical_and(z >= dz, jnp.logical_not(homed)))
                def _():
                    pl.semaphore_signal(seen, inc=1, device_id=at(z - dz, dx, dg), device_id_type=MESH)

    for h in range(nh // LANES):
        hubcol[h * LANES:(h + 1) * LANES, :] = jnp.transpose(
            jnp.broadcast_to(ids_ref[h:h + 1, :], (LANES, LANES)))

    def hub_hits(base):
        return hubcol[...] == base + lax.broadcasted_iota(jnp.int32, (nh, LANES), 1)

    def light_lanes(t, carry):
        hit = jnp.max(jnp.where(hub_hits(t * LANES), 1, 0), axis=0, keepdims=True)
        keep[pl.ds(t, 1), :] = hit - 1
        return carry

    tiles = bc // LANES
    lax.fori_loop(0, C * tiles, light_lanes, 0)

    def keep_of(block, first=0, count=tiles):
        return jnp.concatenate([keep[pl.ds(block * tiles + first + t, 1), :] for t in range(count)], axis=1)

    part = pl.ds(pl.multiple_of(g * pc, LANES), pc)

    def wait_row(k):
        pltpu.make_async_copy(rowbuf.at[k], rowbuf.at[k], row_recv.at[k]).wait()

    def wait_hub(slot):
        pltpu.make_async_copy(hubbuf.at[slot], hubbuf.at[slot], hub_recv.at[slot]).wait()

    def wait_cols(plane):
        for mine in range(q):
            @pl.when(jnp.logical_and(plane != r, x == mine))
            def _():
                for tx in range(q):
                    for n, (lo, size) in enumerate(pieces(wq, mine)):
                        ref = colbuf.at[plane, tx, pl.ds(lo - mine * wq // 8 * 8, size), :]
                        pltpu.make_async_copy(ref, ref, col_recv.at[plane, tx, n]).wait()

    def part_keep(tx):
        return keep_of(z * q + tx, g * (pc // LANES), pc // LANES)

    def lanes_of(tx):
        return pl.ds(pl.multiple_of(tx * pc, LANES), pc)

    def load_light(tx):
        kept = part_keep(tx)
        for w in range(bw):
            abuf[32 * w:32 * w + 32, lanes_of(tx)] = spread(
                rowbuf[z * q + tx, w:w + 1, part] & kept, 1.0).astype(BIT)

    def load_hubs(tx):
        kept = part_keep(tx)
        for j in range(G):
            for w in range(hw):
                lo = rows + 32 * (j * hw + w)
                abuf[lo:lo + 32, lanes_of(tx)] = spread(
                    hubbuf[j * C + z * q + tx, w:w + 1, part] & kept, 1.0).astype(BIT)

    def load_b(plane, base):
        first = x * wq - x * wq // 8 * 8
        weight = jnp.where(plane == z, 1.0, 2.0)
        for tx in range(q):
            for w in range(wq):
                bits = colbuf[plane, tx, pl.ds(first + w, 1), part]
                bbuf[base + 32 * w:base + 32 * w + 32, tx * pc:(tx + 1) * pc] = spread(bits, weight).astype(BIT)

        for w in range(hw):
            side[32 * w:32 * w + 32, base:base + bc] = spread(
                hubbuf[g * C + plane * q + x, w:w + 1, :], 2.0).astype(BIT)

    def load_home():
        @pl.when(r > 0)
        def _():
            for dx in range(q):
                wait_hub(g * C + r * q + (x + dx) % q)

        for k in range(q):
            home[k * bc:(k + 1) * bc, :] = jnp.transpose(jnp.concatenate(
                [spread(hubbuf[g * C + r * q + k, w:w + 1, :], 1.0) for w in range(hw)], axis=0)).astype(BIT)

    def multiply(planes):
        deep = len(planes) * bc
        for n, plane in enumerate(planes):
            load_b(plane, n * bc)
        all_rows = lax.dot_general(
            abuf[...], bbuf[:deep, :], (((1,), (1,)), ((), ())), preferred_element_type=jnp.float32)
        product[:rows, :deep] = all_rows[:rows, :] + jnp.dot(
            home[...], side[:, :deep], preferred_element_type=jnp.float32)
        product[rows:, :deep] = all_rows[rows:, :]

    def over_lanes(row):
        return functools.reduce(jnp.add, [row[:, t:t + LANES] for t in range(0, row.shape[1], LANES)])

    def close(plane, base):
        k = plane * q + x
        kept = keep_of(k)

        def add(word, lo):
            found = over_lanes(spread(word & kept, product[lo:lo + 32, base:base + bc]))
            wsum[lo:lo + 32, :] += found

        for w in range(bw):
            add(rowbuf[k, w:w + 1, :], 32 * w)
        for j in range(G):
            for w in range(hw):
                add(hubbuf[j * C + k, w:w + 1, :], rows + 32 * (j * hw + w))

    wsum[...] = jnp.zeros_like(wsum)
    load_light(x)
    for t in range(rows // LANES):
        lanes = slice(t * LANES, (t + 1) * LANES)
        hits = jnp.where(hub_hits(r * rows + t * LANES), 1.0, 0.0)
        owner[:, lanes] = hits
        light[:, lanes] = 1.0 - jnp.sum(hits, axis=0, keepdims=True)

    for dg in range(1, G):
        wait_hub((g + dg) % G * C + c)
    load_hubs(x)

    kept = part_keep(x)
    hub_deg = jnp.sum(jnp.concatenate([
        over_lanes(spread(hubbuf[j * C + c, w:w + 1, part] & kept, 1.0)) for j in range(G) for w in range(hw)],
        axis=0), axis=1, keepdims=True)

    def turn(matrix):
        ones = jnp.ones((8, matrix.shape[1]), matrix.dtype)
        return lax.dot_general(
            ones, matrix, (((1,), (1,)), ((), ())), preferred_element_type=jnp.float32)[:1, :]

    def owned(row, column):
        return light[...] * row + jnp.sum(owner[...] * column, axis=0, keepdims=True)

    def post(row, value):
        for slot in range(G * C):
            to = slot % C
            outbox[slot, row:row + 1, :per] = value[:, to * per:(to + 1) * per]

    deg_row = owned(turn(abuf[:rows, lanes_of(x)]), hub_deg)
    post(1, deg_row)

    for dx in range(1, q):
        other = (x + dx) % q
        for dg in range(G):
            wait_hub((g + dg) % G * C + z * q + other)
        load_hubs(other)
    for dx in range(1, q):
        other = (x + dx) % q
        wait_row(z * q + other)
        load_light(other)

    base = x * wq // 8 * 8
    for tx in range(q):
        colbuf[r, tx] = rowbuf[z * q + tx, pl.ds(pl.multiple_of(base, 8), colbuf.shape[2]), :]

    @pl.when(z > 0)
    def _():
        home[...] = jnp.zeros((rows, ng), BIT)

    @pl.when(z == 0)
    def _():
        load_home()

        @pl.when(x == 0)
        def _():
            extra = light[...] * jnp.concatenate([
                jnp.sum(functools.reduce(jnp.add, [
                    spread(hubbuf[g * C + r * q + k, w:w + 1, :], 1.0) for w in range(hw)]), axis=0, keepdims=True)
                for k in range(q)], axis=1)
            post(1, deg_row + extra)

    def wait_hubs(plane):
        for dg in range(G):
            @pl.when(jnp.logical_and(plane > z, jnp.logical_not(jnp.logical_and(z == 0, plane == r)))
                     if dg == 0 else plane > z)
            def _():
                wait_hub((g + dg) % G * C + plane * q + x)

    def steps(planes):
        for plane in planes:
            wait_cols(plane)
            wait_hubs(plane)
        multiply(planes)
        for n, plane in enumerate(planes):
            pl.when(plane > z)(functools.partial(wait_row, plane * q + x))
            close(plane, n * bc)

    odd = (R - z) % 2

    @pl.when(odd == 1)
    def _():
        steps([z])

    def pair(n, carry):
        first = z + odd + 2 * n
        steps([first, first + 1])
        return carry

    lax.fori_loop(0, (R - z) // 2, pair, 0)

    hub_tri = jnp.sum(wsum[rows:, :], axis=1, keepdims=True)
    rest = wsum[:rows, :]
    tri_row = jnp.zeros((1, rows), jnp.float32)
    for _ in range(3):
        upper = rest.astype(jnp.bfloat16)
        tri_row = tri_row + turn(upper)
        rest = rest - upper.astype(jnp.float32)
    post(0, owned(tri_row, hub_tri))

    def message(slot):
        return pltpu.make_async_remote_copy(
            src_ref=outbox.at[slot], dst_ref=inbox.at[me], send_sem=msg_send.at[slot], recv_sem=msg_recv.at[me],
            device_id=(r, slot % C, slot // C), device_id_type=MESH)

    def messages(act):
        for slot in range(G * C):
            @pl.when(slot != me)
            def _():
                act(message(slot))

    @pl.when(z < R - 1)
    def _():
        pl.semaphore_wait(seen, (R - 1 - z) * (q - 1) * G - jnp.where(jnp.logical_and(z == 0, r > 0), q - 1, 0))

    messages(lambda copy: copy.start())
    tri = outbox[me, 0:1, :]
    deg = outbox[me, 1:2, :]
    for d in range(1, G * C):
        slot = (me + d) % (G * C)
        pltpu.make_async_copy(inbox.at[slot], inbox.at[slot], msg_recv.at[slot]).wait()
        tri = tri + inbox[slot, 0:1, :]
        deg = deg + inbox[slot, 1:2, :]
    out_ref[...] = (0.5 * tri / (1.0 + deg))[:, :per]
    moves(lambda copy: copy.wait_send())
    messages(lambda copy: copy.wait_send())


def body(light_bits, hub_bits, hub_ids):
    R, C, G = lax.axis_size("rows"), lax.axis_size("cols"), lax.axis_size("hub")
    bw, bc = light_bits.shape
    hw = hub_bits.shape[0]
    nh = hub_ids.shape[0]
    rows, pc = 32 * bw, bc // G
    per = rows // C
    q = C // R
    size, count = shape_of(bw // q, q)
    dma = pltpu.SemaphoreType.DMA
    hbm = pl.BlockSpec(memory_space=pltpu.HBM)
    buffers = [
        ((nh // LANES, LANES), jnp.int32),
        ((C, bw, bc), jnp.int32),
        ((R, q, size, bc), jnp.int32),
        ((G * C, hw, bc), jnp.int32),
        ((C * bc // LANES, LANES), jnp.int32),
        ((nh, LANES), jnp.int32),
        ((rows + nh, q * pc), BIT),
        ((2 * bc, q * pc), BIT),
        ((rows, nh // G), BIT),
        ((nh // G, 2 * bc), BIT),
        ((nh, rows), jnp.float32),
        ((1, rows), jnp.float32),
        ((rows + nh, 2 * bc), jnp.float32),
        ((rows + nh, LANES), jnp.float32),
        ((G * C, 2, LANES), jnp.float32),
        ((G * C, 2, LANES), jnp.float32),
    ]
    held = sum(math.prod(shape) * jnp.dtype(dtype).itemsize for shape, dtype in buffers)
    held += 8 * (rows + nh) * bc
    out = pl.pallas_call(
        functools.partial(kernel, R, C, G),
        out_shape=jax.ShapeDtypeStruct((1, per), jnp.float32),
        in_specs=[hbm, hbm, hbm],
        out_specs=pl.BlockSpec(memory_space=pltpu.VMEM),
        scratch_shapes=[pltpu.VMEM(shape, dtype) for shape, dtype in buffers] + [
            dma((3,)), dma((R, q)), dma((C,)), dma((R, q, count)), dma((R, q, count)),
            dma((R + 1, q, G)), dma((G * C,)), dma((G * C,)), dma((G * C,)), pltpu.SemaphoreType.REGULAR,
        ],
        compiler_params=pltpu.CompilerParams(
            collective_id=0, has_side_effects=True, vmem_limit_bytes=held + 12 * 1024 * 1024),
    )(*(pltpu.with_memory_space_constraint(x, pltpu.HBM)
        for x in (light_bits, hub_bits, hub_ids.reshape(nh // LANES, LANES))))
    return out.reshape(per)


def solution(mesh):
    return jax.shard_map(
        body,
        mesh=mesh,
        in_specs=(P("rows", "cols"), P("hub", "cols"), P()),
        out_specs=P(("rows", "cols")),
        check_vma=False,
    )
```

```python
import functools
import math

import jax
import jax.numpy as jnp
from jax import lax
from jax.experimental import pallas as pl
from jax.experimental.pallas import tpu as pltpu
from jax.sharding import PartitionSpec as P

LANES = 128
BIT = jnp.float8_e4m3fn
MESH = pl.DeviceIdType.MESH


def spread(row, value, other=0.0):
    masks = jnp.left_shift(jnp.int32(1), lax.broadcasted_iota(jnp.int32, (32, row.shape[1]), 0))
    return jnp.where((jnp.broadcast_to(row, masks.shape) & masks) != 0, value, other)


def pieces(wq, x):
    cuts = [x * wq] + [t for t in range(8, (x + 1) * wq, 8) if t > x * wq] + [(x + 1) * wq]
    parts = []
    for lo, hi in zip(cuts, cuts[1:]):
        if parts and lo % 8 == 0 and hi % 8 == 0 and parts[-1][0] % 8 == 0 and sum(parts[-1]) == lo:
            parts[-1] = (parts[-1][0], hi - parts[-1][0])
        else:
            parts.append((lo, hi - lo))
    return parts


def shape_of(wq, q):
    size = max(-(-(x + 1) * wq // 8) * 8 - x * wq // 8 * 8 for x in range(q))
    return size, max(len(pieces(wq, x)) for x in range(q))


def kernel(
    R, C, G,
    light_hbm, hub_hbm, ids_hbm, out_ref,
    ids_ref, rowbuf, colbuf, hubbuf, keep, hubcol, abuf, bbuf, owner, light, product, wsum, outbox, inbox,
    local_sem, row_send, row_recv, col_send, col_recv, hub_send, hub_recv, msg_send, msg_recv, seen,
):
    r, c, g = lax.axis_index("rows"), lax.axis_index("cols"), lax.axis_index("hub")
    _, bw, bc = rowbuf.shape
    hw = hubbuf.shape[1]
    pc = bc // G
    q = C // R
    z, x = c // q, c % q
    rows = 32 * bw
    wq = bw // q
    ng = 32 * hw
    nh = ng * G
    per = rows // C
    me = g * C + c

    own = [
        pltpu.make_async_copy(light_hbm, rowbuf.at[c], local_sem.at[0]),
        pltpu.make_async_copy(hub_hbm, hubbuf.at[me], local_sem.at[1]),
        pltpu.make_async_copy(ids_hbm, ids_ref, local_sem.at[2]),
    ]
    for copy in own:
        copy.start()

    def at(plane, dx, dg=0):
        return (r, plane * q + (x + dx) % q, (g + dg) % G)

    barrier = pltpu.get_barrier_semaphore()

    def greet(device):
        pl.semaphore_signal(barrier, inc=1, device_id=device, device_id_type=MESH)

    for dz in range(R):
        @pl.when(z + dz < R)
        def _():
            for dx in range(q):
                for dg in range(G):
                    if dz or dx or dg:
                        greet(at(z + dz, dx, dg))
    for dr in range(1, R):
        @pl.when((r + dr) % R >= z)
        def _():
            for dx in range(q):
                greet(((r + dr) % R, z * q + dx, g))

    def row_copy(dz, dx):
        return pltpu.make_async_remote_copy(
            src_ref=rowbuf.at[c], dst_ref=rowbuf.at[c], send_sem=row_send.at[dz, dx], recv_sem=row_recv.at[c],
            device_id=at(z - dz, dx), device_id_type=MESH)

    def hub_copy(dz, dx, dg):
        return pltpu.make_async_remote_copy(
            src_ref=hubbuf.at[me], dst_ref=hubbuf.at[me], send_sem=hub_send.at[dz, dx, dg],
            recv_sem=hub_recv.at[me], device_id=at(z - dz, dx, dg), device_id_type=MESH)

    def homing(dx):
        return pltpu.make_async_remote_copy(
            src_ref=hubbuf.at[me], dst_ref=hubbuf.at[me], send_sem=hub_send.at[R, dx, 0],
            recv_sem=hub_recv.at[me], device_id=at(0, dx), device_id_type=MESH)

    def col_copies(to, tx):
        base = tx * wq // 8 * 8
        return [
            pltpu.make_async_remote_copy(
                src_ref=rowbuf.at[c, pl.ds(lo, size), :], dst_ref=colbuf.at[r, x, pl.ds(lo - base, size), :],
                send_sem=col_send.at[to, tx, n], recv_sem=col_recv.at[r, x, n],
                device_id=(to, z * q + tx, g), device_id_type=MESH)
            for n, (lo, size) in enumerate(pieces(wq, tx))]

    def send_cols(act, targets):
        @pl.when(r >= z)
        def _():
            for to in targets:
                @pl.when(r != to)
                def _():
                    for tx in range(q):
                        for copy in col_copies(to, tx):
                            act(copy)

    def send_near(act):
        @pl.when(jnp.logical_and(z == r, z > 0))
        def _():
            for dx in range(1, q):
                act(homing(dx))

        send_cols(act, range(1))
        for dx in range(q):
            for dg in range(G):
                if dx or dg:
                    act(hub_copy(0, dx, dg))
        for dx in range(1, q):
            act(row_copy(0, dx))

    def send_far(act):
        for dz in [1] + list(range(R - 1, 1, -1)):
            @pl.when(z >= dz)
            def _():
                for dg in range(G):
                    act(hub_copy(dz, 0, dg))
                act(row_copy(dz, 0))

    def moves(act):
        send_near(act)
        send_far(act)
        send_cols(act, range(1, R))

    for copy in own:
        copy.wait()
    pl.semaphore_wait(barrier, (z + 1) * q * G - 1 + jnp.where(r >= z, (R - 1) * q, 0))
    def start(copy):
        copy.start()

    send_near(start)
    send_far(start)
    send_cols(start, range(1, R))
    for dz in range(1, R):
        for dx in range(1, q):
            for dg in range(G):
                homed = jnp.logical_and(z == r, z == dz) if dg == 0 else False

                @pl.when(jnp.logical_and(z >= dz, jnp.logical_not(homed)))
                def _():
                    pl.semaphore_signal(seen, inc=1, device_id=at(z - dz, dx, dg), device_id_type=MESH)

    for h in range(nh // LANES):
        hubcol[h * LANES:(h + 1) * LANES, :] = jnp.transpose(
            jnp.broadcast_to(ids_ref[h:h + 1, :], (LANES, LANES)))

    def hub_hits(base):
        return hubcol[...] == base + lax.broadcasted_iota(jnp.int32, (nh, LANES), 1)

    def light_lanes(t, carry):
        hit = jnp.max(jnp.where(hub_hits(t * LANES), 1, 0), axis=0, keepdims=True)
        keep[pl.ds(t, 1), :] = hit - 1
        return carry

    tiles = bc // LANES
    lax.fori_loop(0, C * tiles, light_lanes, 0)

    def keep_of(block, first=0, count=tiles):
        return jnp.concatenate([keep[pl.ds(block * tiles + first + t, 1), :] for t in range(count)], axis=1)

    part = pl.ds(pl.multiple_of(g * pc, LANES), pc)

    def wait_row(k):
        pltpu.make_async_copy(rowbuf.at[k], rowbuf.at[k], row_recv.at[k]).wait()

    def wait_hub(slot):
        pltpu.make_async_copy(hubbuf.at[slot], hubbuf.at[slot], hub_recv.at[slot]).wait()

    def wait_cols(plane):
        for mine in range(q):
            @pl.when(jnp.logical_and(plane != r, x == mine))
            def _():
                for tx in range(q):
                    for n, (lo, size) in enumerate(pieces(wq, mine)):
                        ref = colbuf.at[plane, tx, pl.ds(lo - mine * wq // 8 * 8, size), :]
                        pltpu.make_async_copy(ref, ref, col_recv.at[plane, tx, n]).wait()

    def part_keep(tx):
        return keep_of(z * q + tx, g * (pc // LANES), pc // LANES)

    def lanes_of(tx):
        return pl.ds(pl.multiple_of(tx * pc, LANES), pc)

    def load_light(tx):
        kept = part_keep(tx)
        for w in range(bw):
            abuf[32 * w:32 * w + 32, lanes_of(tx)] = spread(
                rowbuf[z * q + tx, w:w + 1, part] & kept, 1.0).astype(BIT)

    def load_hubs(tx):
        kept = part_keep(tx)
        for j in range(G):
            for w in range(hw):
                lo = rows + 32 * (j * hw + w)
                abuf[lo:lo + 32, lanes_of(tx)] = spread(
                    hubbuf[j * C + z * q + tx, w:w + 1, part] & kept, 1.0).astype(BIT)

    def load_b(plane, base, hubs):
        first = x * wq - x * wq // 8 * 8
        weight = jnp.where(plane == z, 1.0, 2.0)
        for tx in range(q):
            for w in range(wq):
                bits = colbuf[plane, tx, pl.ds(first + w, 1), part]
                bbuf[base + 32 * w:base + 32 * w + 32, tx * pc:(tx + 1) * pc] = spread(bits, weight).astype(BIT)
        if hubs:
            bbuf[base:base + bc, q * pc:] = hub_rows(plane * q + x, 2.0)

    def hub_rows(block, value):
        return jnp.transpose(jnp.concatenate(
            [spread(hubbuf[g * C + block, w:w + 1, :], value) for w in range(hw)], axis=0)).astype(BIT)

    def load_home():
        @pl.when(r > 0)
        def _():
            for dx in range(q):
                wait_hub(g * C + r * q + (x + dx) % q)

        for k in range(q):
            abuf[k * bc:(k + 1) * bc, q * pc:] = hub_rows(r * q + k, 1.0)
        abuf[rows:, q * pc:] = jnp.zeros((nh, ng), BIT)

    def multiply(planes, hubs):
        deep = len(planes) * bc
        for n, plane in enumerate(planes):
            load_b(plane, n * bc, hubs)
        wide = q * pc + (ng if hubs else 0)
        product[:, :deep] = lax.dot_general(
            abuf[:, :wide], bbuf[:deep, :wide], (((1,), (1,)), ((), ())), preferred_element_type=jnp.float32)
        close(planes[0], 0)

    def over_lanes(row):
        return functools.reduce(jnp.add, [row[:, t:t + LANES] for t in range(0, row.shape[1], LANES)])

    def close(plane, base):
        k = plane * q + x
        kept = keep_of(k)

        def add(word, lo):
            found = over_lanes(spread(word & kept, product[lo:lo + 32, base:base + bc]))
            wsum[lo:lo + 32, :] += found

        for w in range(bw):
            add(rowbuf[k, w:w + 1, :], 32 * w)
        for j in range(G):
            for w in range(hw):
                add(hubbuf[j * C + k, w:w + 1, :], rows + 32 * (j * hw + w))

    wsum[...] = jnp.zeros_like(wsum)
    load_light(x)
    for t in range(rows // LANES):
        lanes = slice(t * LANES, (t + 1) * LANES)
        hits = jnp.where(hub_hits(r * rows + t * LANES), 1.0, 0.0)
        owner[:, lanes] = hits
        light[:, lanes] = 1.0 - jnp.sum(hits, axis=0, keepdims=True)

    for dg in range(1, G):
        wait_hub((g + dg) % G * C + c)
    load_hubs(x)

    kept = part_keep(x)
    hub_deg = jnp.sum(jnp.concatenate([
        over_lanes(spread(hubbuf[j * C + c, w:w + 1, part] & kept, 1.0)) for j in range(G) for w in range(hw)],
        axis=0), axis=1, keepdims=True)

    def turn(matrix):
        ones = jnp.ones((8, matrix.shape[1]), matrix.dtype)
        return lax.dot_general(
            ones, matrix, (((1,), (1,)), ((), ())), preferred_element_type=jnp.float32)[:1, :]

    def owned(row, column):
        return light[...] * row + jnp.sum(owner[...] * column, axis=0, keepdims=True)

    def post(row, value):
        for slot in range(G * C):
            to = slot % C
            outbox[slot, row:row + 1, :per] = value[:, to * per:(to + 1) * per]

    deg_row = owned(turn(abuf[:rows, lanes_of(x)]), hub_deg)
    post(1, deg_row)

    for dx in range(1, q):
        other = (x + dx) % q
        for dg in range(G):
            wait_hub((g + dg) % G * C + z * q + other)
        load_hubs(other)
    for dx in range(1, q):
        other = (x + dx) % q
        wait_row(z * q + other)
        load_light(other)

    base = x * wq // 8 * 8
    for tx in range(q):
        colbuf[r, tx] = rowbuf[z * q + tx, pl.ds(pl.multiple_of(base, 8), colbuf.shape[2]), :]

    @pl.when(z == 0)
    def _():
        load_home()

        @pl.when(x == 0)
        def _():
            extra = light[...] * jnp.concatenate([
                jnp.sum(functools.reduce(jnp.add, [
                    spread(hubbuf[g * C + r * q + k, w:w + 1, :], 1.0) for w in range(hw)]), axis=0, keepdims=True)
                for k in range(q)], axis=1)
            post(1, deg_row + extra)

    def wait_hubs(plane):
        for dg in range(G):
            @pl.when(jnp.logical_and(plane > z, jnp.logical_not(jnp.logical_and(z == 0, plane == r)))
                     if dg == 0 else plane > z)
            def _():
                wait_hub((g + dg) % G * C + plane * q + x)

    def meet_row(plane):
        pl.when(plane > z)(functools.partial(wait_row, plane * q + x))

    odd = (R - z) % 2

    @pl.when(odd == 1)
    def _():
        wait_cols(z)
        multiply([z], R % 2 == 1)

    def pair(n, carry):
        planes = [z + odd + 2 * n, z + odd + 2 * n + 1]
        for plane in planes:
            wait_cols(plane)
            wait_hubs(plane)
        meet_row(planes[0])
        pl.when(z == 0)(functools.partial(multiply, planes, True))
        pl.when(z > 0)(functools.partial(multiply, planes, False))
        wait_row(planes[1] * q + x)
        close(planes[1], bc)
        return carry

    lax.fori_loop(0, (R - z) // 2, pair, 0)

    hub_tri = jnp.sum(wsum[rows:, :], axis=1, keepdims=True)
    rest = wsum[:rows, :]
    tri_row = jnp.zeros((1, rows), jnp.float32)
    largest = 2 * (q * pc + ng) * R * (bc // LANES)
    for _ in range(-(-largest.bit_length() // 8)):
        upper = rest.astype(jnp.bfloat16)
        tri_row = tri_row + turn(upper)
        rest = rest - upper.astype(jnp.float32)
    post(0, owned(tri_row, hub_tri))

    def message(slot):
        return pltpu.make_async_remote_copy(
            src_ref=outbox.at[slot], dst_ref=inbox.at[me], send_sem=msg_send.at[slot], recv_sem=msg_recv.at[me],
            device_id=(r, slot % C, slot // C), device_id_type=MESH)

    def messages(act):
        for slot in range(G * C):
            @pl.when(slot != me)
            def _():
                act(message(slot))

    @pl.when(z < R - 1)
    def _():
        pl.semaphore_wait(seen, (R - 1 - z) * (q - 1) * G - jnp.where(jnp.logical_and(z == 0, r > 0), q - 1, 0))

    messages(lambda copy: copy.start())
    tri = outbox[me, 0:1, :]
    deg = outbox[me, 1:2, :]
    for d in range(1, G * C):
        slot = (me + d) % (G * C)
        pltpu.make_async_copy(inbox.at[slot], inbox.at[slot], msg_recv.at[slot]).wait()
        tri = tri + inbox[slot, 0:1, :]
        deg = deg + inbox[slot, 1:2, :]
    out_ref[...] = (0.5 * tri / (1.0 + deg))[:, :per]
    moves(lambda copy: copy.wait_send())
    messages(lambda copy: copy.wait_send())


def body(light_bits, hub_bits, hub_ids):
    R, C, G = lax.axis_size("rows"), lax.axis_size("cols"), lax.axis_size("hub")
    bw, bc = light_bits.shape
    hw = hub_bits.shape[0]
    nh = hub_ids.shape[0]
    rows, pc = 32 * bw, bc // G
    per = rows // C
    q = C // R
    size, count = shape_of(bw // q, q)
    dma = pltpu.SemaphoreType.DMA
    hbm = pl.BlockSpec(memory_space=pltpu.HBM)
    buffers = [
        ((nh // LANES, LANES), jnp.int32),
        ((C, bw, bc), jnp.int32),
        ((R, q, size, bc), jnp.int32),
        ((G * C, hw, bc), jnp.int32),
        ((C * bc // LANES, LANES), jnp.int32),
        ((nh, LANES), jnp.int32),
        ((rows + nh, q * pc + nh // G), BIT),
        ((2 * bc, q * pc + nh // G), BIT),
        ((nh, rows), jnp.float32),
        ((1, rows), jnp.float32),
        ((rows + nh, 2 * bc), jnp.float32),
        ((rows + nh, LANES), jnp.float32),
        ((G * C, 2, LANES), jnp.float32),
        ((G * C, 2, LANES), jnp.float32),
    ]
    held = sum(math.prod(shape) * jnp.dtype(dtype).itemsize for shape, dtype in buffers)
    held += 8 * (rows + nh) * bc
    out = pl.pallas_call(
        functools.partial(kernel, R, C, G),
        out_shape=jax.ShapeDtypeStruct((1, per), jnp.float32),
        in_specs=[hbm, hbm, hbm],
        out_specs=pl.BlockSpec(memory_space=pltpu.VMEM),
        scratch_shapes=[pltpu.VMEM(shape, dtype) for shape, dtype in buffers] + [
            dma((3,)), dma((R, q)), dma((C,)), dma((R, q, count)), dma((R, q, count)),
            dma((R + 1, q, G)), dma((G * C,)), dma((G * C,)), dma((G * C,)), pltpu.SemaphoreType.REGULAR,
        ],
        compiler_params=pltpu.CompilerParams(
            collective_id=0, has_side_effects=True, vmem_limit_bytes=held + 12 * 1024 * 1024),
    )(*(pltpu.with_memory_space_constraint(x, pltpu.HBM)
        for x in (light_bits, hub_bits, hub_ids.reshape(nh // LANES, LANES))))
    return out.reshape(per)


def solution(mesh):
    return jax.shard_map(
        body,
        mesh=mesh,
        in_specs=(P("rows", "cols"), P("hub", "cols"), P()),
        out_specs=P(("rows", "cols")),
        check_vma=False,
    )
```

```python
import functools
import math

import jax
import jax.numpy as jnp
from jax import lax
from jax.experimental import pallas as pl
from jax.experimental.pallas import tpu as pltpu
from jax.sharding import PartitionSpec as P

LANES = 128
BIT = jnp.float8_e4m3fn
MESH = pl.DeviceIdType.MESH


def spread(row, value, other=0.0):
    masks = jnp.left_shift(jnp.int32(1), lax.broadcasted_iota(jnp.int32, (32, row.shape[1]), 0))
    return jnp.where((jnp.broadcast_to(row, masks.shape) & masks) != 0, value, other)


def pieces(wq, x):
    cuts = [x * wq] + [t for t in range(8, (x + 1) * wq, 8) if t > x * wq] + [(x + 1) * wq]
    parts = []
    for lo, hi in zip(cuts, cuts[1:]):
        if parts and lo % 8 == 0 and hi % 8 == 0 and parts[-1][0] % 8 == 0 and sum(parts[-1]) == lo:
            parts[-1] = (parts[-1][0], hi - parts[-1][0])
        else:
            parts.append((lo, hi - lo))
    return parts


def shape_of(wq, q):
    size = max(-(-(x + 1) * wq // 8) * 8 - x * wq // 8 * 8 for x in range(q))
    return size, max(len(pieces(wq, x)) for x in range(q))


def kernel(
    R, C, G,
    light_hbm, hub_hbm, ids_hbm, out_ref,
    ids_ref, rowbuf, colbuf, hubbuf, keep, hubcol, abuf, bbuf, owner, light, product, wsum, outbox, inbox,
    local_sem, row_send, row_recv, col_send, col_recv, hub_send, hub_recv, msg_send, msg_recv, seen,
):
    r, c, g = lax.axis_index("rows"), lax.axis_index("cols"), lax.axis_index("hub")
    _, bw, bc = rowbuf.shape
    hw = hubbuf.shape[1]
    pc = bc // G
    q = C // R
    z, x = c // q, c % q
    rows = 32 * bw
    wq = bw // q
    ng = 32 * hw
    nh = ng * G
    per = rows // C
    lead = -(-per // LANES) * LANES
    front = nh + lead
    me = g * C + c

    own = [
        pltpu.make_async_copy(light_hbm, rowbuf.at[c], local_sem.at[0]),
        pltpu.make_async_copy(hub_hbm, hubbuf.at[me], local_sem.at[1]),
        pltpu.make_async_copy(ids_hbm, ids_ref, local_sem.at[2]),
    ]
    for copy in own:
        copy.start()

    def at(plane, dx, dg=0):
        return (r, plane * q + (x + dx) % q, (g + dg) % G)

    barrier = pltpu.get_barrier_semaphore()

    def greet(device):
        pl.semaphore_signal(barrier, inc=1, device_id=device, device_id_type=MESH)

    for dz in range(R):
        @pl.when(z + dz < R)
        def _():
            for dx in range(q):
                for dg in range(G):
                    if dz or dx or dg:
                        greet(at(z + dz, dx, dg))
    for dr in range(1, R):
        @pl.when((r + dr) % R >= z)
        def _():
            for dx in range(q):
                greet(((r + dr) % R, z * q + dx, g))

    def row_copy(dz, dx):
        return pltpu.make_async_remote_copy(
            src_ref=rowbuf.at[c], dst_ref=rowbuf.at[c], send_sem=row_send.at[dz, dx], recv_sem=row_recv.at[c],
            device_id=at(z - dz, dx), device_id_type=MESH)

    def hub_copy(dz, dx, dg):
        return pltpu.make_async_remote_copy(
            src_ref=hubbuf.at[me], dst_ref=hubbuf.at[me], send_sem=hub_send.at[dz, dx, dg],
            recv_sem=hub_recv.at[me], device_id=at(z - dz, dx, dg), device_id_type=MESH)

    def homing(dx):
        return pltpu.make_async_remote_copy(
            src_ref=hubbuf.at[me], dst_ref=hubbuf.at[me], send_sem=hub_send.at[R, dx, 0],
            recv_sem=hub_recv.at[me], device_id=at(0, dx), device_id_type=MESH)

    def col_copies(to, tx):
        base = tx * wq // 8 * 8
        return [
            pltpu.make_async_remote_copy(
                src_ref=rowbuf.at[c, pl.ds(lo, size), :], dst_ref=colbuf.at[r, x, pl.ds(lo - base, size), :],
                send_sem=col_send.at[to, tx, n], recv_sem=col_recv.at[r, x, n],
                device_id=(to, z * q + tx, g), device_id_type=MESH)
            for n, (lo, size) in enumerate(pieces(wq, tx))]

    def send_cols(act, targets):
        @pl.when(r >= z)
        def _():
            for to in targets:
                @pl.when(r != to)
                def _():
                    for tx in range(q):
                        for copy in col_copies(to, tx):
                            act(copy)

    def send_near(act):
        @pl.when(jnp.logical_and(z == r, z > 0))
        def _():
            for dx in range(1, q):
                act(homing(dx))

        send_cols(act, range(1))
        for dx in range(q):
            for dg in range(G):
                if dx or dg:
                    act(hub_copy(0, dx, dg))
        for dx in range(1, q):
            act(row_copy(0, dx))

    def send_far(act):
        for dz in [1] + list(range(R - 1, 1, -1)):
            @pl.when(z >= dz)
            def _():
                for dg in range(G):
                    act(hub_copy(dz, 0, dg))
                act(row_copy(dz, 0))

    def moves(act):
        send_near(act)
        send_far(act)
        send_cols(act, range(1, R))

    for copy in own:
        copy.wait()
    pl.semaphore_wait(barrier, (z + 1) * q * G - 1 + jnp.where(r >= z, (R - 1) * q, 0))
    def start(copy):
        copy.start()

    send_near(start)
    send_far(start)
    send_cols(start, range(1, R))
    for dz in range(1, R):
        for dx in range(1, q):
            for dg in range(G):
                homed = jnp.logical_and(z == r, z == dz) if dg == 0 else False

                @pl.when(jnp.logical_and(z >= dz, jnp.logical_not(homed)))
                def _():
                    pl.semaphore_signal(seen, inc=1, device_id=at(z - dz, dx, dg), device_id_type=MESH)

    for h in range(nh // LANES):
        hubcol[h * LANES:(h + 1) * LANES, :] = jnp.transpose(
            jnp.broadcast_to(ids_ref[h:h + 1, :], (LANES, LANES)))

    def hub_hits(base):
        return hubcol[...] == base + lax.broadcasted_iota(jnp.int32, (nh, LANES), 1)

    def light_lanes(t, carry):
        hit = jnp.max(jnp.where(hub_hits(t * LANES), 1, 0), axis=0, keepdims=True)
        keep[pl.ds(t, 1), :] = hit - 1
        return carry

    tiles = bc // LANES
    lax.fori_loop(0, C * tiles, light_lanes, 0)

    def keep_of(block, first=0, count=tiles):
        return jnp.concatenate([keep[pl.ds(block * tiles + first + t, 1), :] for t in range(count)], axis=1)

    part = pl.ds(pl.multiple_of(g * pc, LANES), pc)

    def wait_row(k):
        pltpu.make_async_copy(rowbuf.at[k], rowbuf.at[k], row_recv.at[k]).wait()

    def wait_hub(slot):
        pltpu.make_async_copy(hubbuf.at[slot], hubbuf.at[slot], hub_recv.at[slot]).wait()

    def wait_cols(plane):
        for mine in range(q):
            @pl.when(jnp.logical_and(plane != r, x == mine))
            def _():
                for tx in range(q):
                    for n, (lo, size) in enumerate(pieces(wq, mine)):
                        ref = colbuf.at[plane, tx, pl.ds(lo - mine * wq // 8 * 8, size), :]
                        pltpu.make_async_copy(ref, ref, col_recv.at[plane, tx, n]).wait()

    def part_keep(tx):
        return keep_of(z * q + tx, g * (pc // LANES), pc // LANES)

    def lanes_of(tx):
        return pl.ds(pl.multiple_of(tx * pc, LANES), pc)

    def load_light(tx):
        kept = part_keep(tx)
        for w in range(bw):
            abuf[nh + 32 * w:nh + 32 * w + 32, lanes_of(tx)] = spread(
                rowbuf[z * q + tx, w:w + 1, part] & kept, 1.0).astype(BIT)

    def load_hubs(tx):
        kept = part_keep(tx)
        for j in range(G):
            for w in range(hw):
                lo = 32 * (j * hw + w)
                abuf[lo:lo + 32, lanes_of(tx)] = spread(
                    hubbuf[j * C + z * q + tx, w:w + 1, part] & kept, 1.0).astype(BIT)

    def load_b(plane, base, hubs):
        first = x * wq - x * wq // 8 * 8
        weight = jnp.where(plane == z, 1.0, 2.0)
        for tx in range(q):
            for w in range(wq):
                bits = colbuf[plane, tx, pl.ds(first + w, 1), part]
                bbuf[base + 32 * w:base + 32 * w + 32, tx * pc:(tx + 1) * pc] = spread(bits, weight).astype(BIT)
        if hubs:
            bbuf[base:base + bc, q * pc:] = hub_rows(plane * q + x, 2.0)

    def hub_rows(block, value):
        return jnp.transpose(jnp.concatenate(
            [spread(hubbuf[g * C + block, w:w + 1, :], value) for w in range(hw)], axis=0)).astype(BIT)

    def load_home():
        @pl.when(r > 0)
        def _():
            for dx in range(q):
                wait_hub(g * C + r * q + (x + dx) % q)

        for k in range(q):
            abuf[nh + k * bc:nh + (k + 1) * bc, q * pc:] = hub_rows(r * q + k, 1.0)

    def multiply(planes, base, hubs):
        wide = q * pc + (ng if hubs else 0)
        for n, plane in enumerate(planes):
            load_b(plane, n * bc, hubs)
        deep = len(planes) * bc
        product[:, base:base + deep] = lax.dot_general(
            abuf[:, :wide], bbuf[:deep, :wide], (((1,), (1,)), ((), ())), preferred_element_type=jnp.float32)

    def over_lanes(row):
        return functools.reduce(jnp.add, [row[:, t:t + LANES] for t in range(0, row.shape[1], LANES)])

    def close(plane, base, start, stop):
        k = plane * q + x
        kept = keep_of(k)
        words = [(j, w) for j in range(G) for w in range(hw)] + [(G, w) for w in range(bw)]
        for n in range(start // 32, stop // 32):
            j, w = words[n]
            bits = (hubbuf[j * C + k, w:w + 1, :] if j < G else rowbuf[k, w:w + 1, :]) & kept
            at = slice(32 * n, 32 * n + 32)
            wsum[at, :] += over_lanes(spread(bits, product[at, base:base + bc]))

    wsum[...] = jnp.zeros_like(wsum)
    load_light(x)
    for t in range(rows // LANES):
        lanes = slice(t * LANES, (t + 1) * LANES)
        hits = jnp.where(hub_hits(r * rows + t * LANES), 1.0, 0.0)
        owner[:, lanes] = hits
        light[:, lanes] = 1.0 - jnp.sum(hits, axis=0, keepdims=True)

    for dg in range(1, G):
        wait_hub((g + dg) % G * C + c)
    load_hubs(x)

    kept = part_keep(x)
    hub_deg = jnp.sum(jnp.concatenate([
        over_lanes(spread(hubbuf[j * C + c, w:w + 1, part] & kept, 1.0)) for j in range(G) for w in range(hw)],
        axis=0), axis=1, keepdims=True)

    def turn(matrix):
        ones = jnp.ones((8, matrix.shape[1]), matrix.dtype)
        return lax.dot_general(
            ones, matrix, (((1,), (1,)), ((), ())), preferred_element_type=jnp.float32)[:1, :]

    def owned(row, column, start=0):
        lanes = slice(start, start + row.shape[1])
        return light[:, lanes] * row + jnp.sum(owner[:, lanes] * column, axis=0, keepdims=True)

    def post(row, value, owners=range(C)):
        for slot in range(G * C):
            to = slot % C
            if to not in owners:
                continue
            outbox[slot, row:row + 1, :per] = value[:, to * per:(to + 1) * per]

    deg_row = owned(turn(abuf[nh:, lanes_of(x)]), hub_deg)
    post(1, deg_row)

    for dx in range(1, q):
        other = (x + dx) % q
        for dg in range(G):
            wait_hub((g + dg) % G * C + z * q + other)
        load_hubs(other)
    for dx in range(1, q):
        other = (x + dx) % q
        wait_row(z * q + other)
        load_light(other)

    base = x * wq // 8 * 8
    for tx in range(q):
        colbuf[r, tx] = rowbuf[z * q + tx, pl.ds(pl.multiple_of(base, 8), colbuf.shape[2]), :]

    @pl.when(z == 0)
    def _():
        abuf[:nh, q * pc:] = jnp.zeros((nh, ng), BIT)
        load_home()

        @pl.when(x == 0)
        def _():
            extra = light[...] * jnp.concatenate([
                jnp.sum(functools.reduce(jnp.add, [
                    spread(hubbuf[g * C + r * q + k, w:w + 1, :], 1.0) for w in range(hw)]), axis=0, keepdims=True)
                for k in range(q)], axis=1)
            post(1, deg_row + extra)

    def wait_hubs(plane):
        for dg in range(G):
            @pl.when(jnp.logical_and(plane > z, jnp.logical_not(jnp.logical_and(z == 0, plane == r)))
                     if dg == 0 else plane > z)
            def _():
                wait_hub((g + dg) % G * C + plane * q + x)

    def meet_row(plane):
        pl.when(plane > z)(functools.partial(wait_row, plane * q + x))

    odd = (R - z) % 2
    last = R - 1

    @pl.when(odd == 1)
    def _():
        wait_cols(z)

        @pl.when(z < last)
        def _():
            multiply([z], bc, R % 2 == 1)
            close(z, bc, 0, nh + rows)

        @pl.when(z == last)
        def _():
            multiply([z], bc, R == 1)

    def pair(n, carry):
        planes = [z + odd + 2 * n, z + odd + 2 * n + 1]
        for plane in planes:
            wait_cols(plane)
            wait_hubs(plane)
        meet_row(planes[0])
        for hubs, mine in [(True, z == 0), (False, z > 0)]:
            @pl.when(mine)
            def _():
                multiply(planes, 0, hubs)
                close(planes[0], 0, 0, nh + rows)

        wait_row(planes[1] * q + x)

        @pl.when(planes[1] < last)
        def _():
            close(planes[1], bc, 0, nh + rows)

        return carry

    lax.fori_loop(0, (R - z) // 2, pair, 0)
    close(last, bc, 0, front)
    largest = 2 * (q * pc + ng) * R * (bc // LANES)

    def row_sums(start, stop):
        rest = wsum[start:stop, :]
        row = jnp.zeros((1, stop - start), jnp.float32)
        for _ in range(-(-largest.bit_length() // 8)):
            upper = rest.astype(jnp.bfloat16)
            row = row + turn(upper)
            rest = rest - upper.astype(jnp.float32)
        return row

    def message(slot):
        return pltpu.make_async_remote_copy(
            src_ref=outbox.at[slot], dst_ref=inbox.at[me], send_sem=msg_send.at[slot], recv_sem=msg_recv.at[me],
            device_id=(r, slot % C, slot // C), device_id_type=MESH)

    def messages(act, owners):
        for slot in range(G * C):
            if slot % C in owners:
                @pl.when(slot != me)
                def _():
                    act(message(slot))

    hub_tri = jnp.sum(wsum[:nh, :], axis=1, keepdims=True)
    lead_row = owned(row_sums(nh, front), hub_tri)
    for slot in range(0, G * C, C):
        outbox[slot, 0:1, :per] = lead_row[:, :per]
    messages(start, range(1))

    close(last, bc, front, nh + rows)
    later = range(1, C)
    post(0, jnp.concatenate([lead_row, owned(row_sums(front, nh + rows), hub_tri, lead)], axis=1), later)

    @pl.when(z < R - 1)
    def _():
        pl.semaphore_wait(seen, (R - 1 - z) * (q - 1) * G - jnp.where(jnp.logical_and(z == 0, r > 0), q - 1, 0))

    messages(start, later)
    tri = outbox[me, 0:1, :]
    deg = outbox[me, 1:2, :]
    for d in range(1, G * C):
        slot = (me + d) % (G * C)
        pltpu.make_async_copy(inbox.at[slot], inbox.at[slot], msg_recv.at[slot]).wait()
        tri = tri + inbox[slot, 0:1, :]
        deg = deg + inbox[slot, 1:2, :]
    out_ref[...] = (0.5 * tri / (1.0 + deg))[:, :per]
    moves(lambda copy: copy.wait_send())
    messages(lambda copy: copy.wait_send(), range(C))


def body(light_bits, hub_bits, hub_ids):
    R, C, G = lax.axis_size("rows"), lax.axis_size("cols"), lax.axis_size("hub")
    bw, bc = light_bits.shape
    hw = hub_bits.shape[0]
    nh = hub_ids.shape[0]
    rows, pc = 32 * bw, bc // G
    per = rows // C
    q = C // R
    size, count = shape_of(bw // q, q)
    dma = pltpu.SemaphoreType.DMA
    hbm = pl.BlockSpec(memory_space=pltpu.HBM)
    buffers = [
        ((nh // LANES, LANES), jnp.int32),
        ((C, bw, bc), jnp.int32),
        ((R, q, size, bc), jnp.int32),
        ((G * C, hw, bc), jnp.int32),
        ((C * bc // LANES, LANES), jnp.int32),
        ((nh, LANES), jnp.int32),
        ((rows + nh, q * pc + nh // G), BIT),
        ((2 * bc, q * pc + nh // G), BIT),
        ((nh, rows), jnp.float32),
        ((1, rows), jnp.float32),
        ((rows + nh, 2 * bc), jnp.float32),
        ((rows + nh, LANES), jnp.float32),
        ((G * C, 2, LANES), jnp.float32),
        ((G * C, 2, LANES), jnp.float32),
    ]
    held = sum(math.prod(shape) * jnp.dtype(dtype).itemsize for shape, dtype in buffers)
    held += 8 * (rows + nh) * bc
    out = pl.pallas_call(
        functools.partial(kernel, R, C, G),
        out_shape=jax.ShapeDtypeStruct((1, per), jnp.float32),
        in_specs=[hbm, hbm, hbm],
        out_specs=pl.BlockSpec(memory_space=pltpu.VMEM),
        scratch_shapes=[pltpu.VMEM(shape, dtype) for shape, dtype in buffers] + [
            dma((3,)), dma((R, q)), dma((C,)), dma((R, q, count)), dma((R, q, count)),
            dma((R + 1, q, G)), dma((G * C,)), dma((G * C,)), dma((G * C,)), pltpu.SemaphoreType.REGULAR,
        ],
        compiler_params=pltpu.CompilerParams(
            collective_id=0, has_side_effects=True, vmem_limit_bytes=held + 12 * 1024 * 1024),
    )(*(pltpu.with_memory_space_constraint(x, pltpu.HBM)
        for x in (light_bits, hub_bits, hub_ids.reshape(nh // LANES, LANES))))
    return out.reshape(per)


def solution(mesh):
    return jax.shard_map(
        body,
        mesh=mesh,
        in_specs=(P("rows", "cols"), P("hub", "cols"), P()),
        out_specs=P(("rows", "cols")),
        check_vma=False,
    )
```

```python
import functools
import math

import jax
import jax.numpy as jnp
from jax import lax
from jax.experimental import pallas as pl
from jax.experimental.pallas import tpu as pltpu
from jax.sharding import PartitionSpec as P

LANES = 128
BIT = jnp.float8_e4m3fn
MESH = pl.DeviceIdType.MESH


def spread(row, value, other=0.0):
    masks = jnp.left_shift(jnp.int32(1), lax.broadcasted_iota(jnp.int32, (32, row.shape[1]), 0))
    return jnp.where((jnp.broadcast_to(row, masks.shape) & masks) != 0, value, other)


def pieces(wq, x):
    cuts = [x * wq] + [t for t in range(8, (x + 1) * wq, 8) if t > x * wq] + [(x + 1) * wq]
    parts = []
    for lo, hi in zip(cuts, cuts[1:]):
        if parts and lo % 8 == 0 and hi % 8 == 0 and parts[-1][0] % 8 == 0 and sum(parts[-1]) == lo:
            parts[-1] = (parts[-1][0], hi - parts[-1][0])
        else:
            parts.append((lo, hi - lo))
    return parts


def size_of(wq, q):
    return max(-(-(x + 1) * wq // 8) * 8 - x * wq // 8 * 8 for x in range(q))


def kernel(
    R, C, G,
    light_hbm, hub_hbm, ids_hbm, out_ref,
    ids_ref, rowbuf, colbuf, hubbuf, keep, hubcol, abuf, bbuf, owner, light, product, wsum, outbox, inbox,
    local_sem, row_send, row_recv, col_send, col_recv, hub_send, hub_recv, msg_send, msg_recv, seen,
):
    r, c, g = lax.axis_index("rows"), lax.axis_index("cols"), lax.axis_index("hub")
    _, bw, bc = rowbuf.shape
    hw = hubbuf.shape[1]
    pc = bc // G
    q = C // R
    z, x = c // q, c % q
    rows = 32 * bw
    wq = bw // q
    ng = 32 * hw
    nh = ng * G
    per = rows // C
    lead = -(-per // LANES) * LANES
    front = nh + lead
    me = g * C + c

    own = [
        pltpu.make_async_copy(light_hbm, rowbuf.at[c], local_sem.at[0]),
        pltpu.make_async_copy(hub_hbm, hubbuf.at[me], local_sem.at[1]),
        pltpu.make_async_copy(ids_hbm, ids_ref, local_sem.at[2]),
    ]
    for copy in own:
        copy.start()

    def at(plane, dx, dg=0):
        return (r, plane * q + (x + dx) % q, (g + dg) % G)

    barrier = pltpu.get_barrier_semaphore()

    def greet(device):
        pl.semaphore_signal(barrier, inc=1, device_id=device, device_id_type=MESH)

    for dz in range(R):
        @pl.when(z + dz < R)
        def _():
            for dx in range(q):
                for dg in range(G):
                    if dz or dx or dg:
                        greet(at(z + dz, dx, dg))
    for dr in range(1, R):
        @pl.when((r + dr) % R >= z)
        def _():
            for dx in range(q):
                greet(((r + dr) % R, z * q + dx, g))

    def row_copy(dz, dx):
        return pltpu.make_async_remote_copy(
            src_ref=rowbuf.at[c], dst_ref=rowbuf.at[c], send_sem=row_send.at[0], recv_sem=row_recv.at[dz],
            device_id=at(z - dz, dx), device_id_type=MESH)

    def hub_copy(dz, dx, dg):
        return pltpu.make_async_remote_copy(
            src_ref=hubbuf.at[me], dst_ref=hubbuf.at[me], send_sem=hub_send.at[0],
            recv_sem=hub_recv.at[2 + dz if dz else min(dx, 1)], device_id=at(z - dz, dx, dg), device_id_type=MESH)

    def homing(dx):
        return pltpu.make_async_remote_copy(
            src_ref=hubbuf.at[me], dst_ref=hubbuf.at[me], send_sem=hub_send.at[0],
            recv_sem=hub_recv.at[2], device_id=at(0, dx), device_id_type=MESH)

    def col_copies(to, tx):
        base = tx * wq // 8 * 8
        return [
            pltpu.make_async_remote_copy(
                src_ref=rowbuf.at[c, pl.ds(lo, size), :], dst_ref=colbuf.at[r, x, pl.ds(lo - base, size), :],
                send_sem=col_send.at[0], recv_sem=col_recv.at[r],
                device_id=(to, z * q + tx, g), device_id_type=MESH)
            for lo, size in pieces(wq, tx)]

    def send_cols(act, targets):
        @pl.when(r >= z)
        def _():
            for to in targets:
                @pl.when(r != to)
                def _():
                    for tx in range(q):
                        for copy in col_copies(to, tx):
                            act(copy)

    def send_near(act):
        @pl.when(jnp.logical_and(z == r, z > 0))
        def _():
            for dx in range(1, q):
                act(homing(dx))

        send_cols(act, range(1))
        for dx in range(q):
            for dg in range(G):
                if dx or dg:
                    act(hub_copy(0, dx, dg))
        for dx in range(1, q):
            act(row_copy(0, dx))

    def send_far(act):
        for dz in [1] + list(range(R - 1, 1, -1)):
            @pl.when(z >= dz)
            def _():
                for dg in range(G):
                    act(hub_copy(dz, 0, dg))
                act(row_copy(dz, 0))

    def drain(buffer, count, sem):
        if count:
            ref = buffer.at[pl.ds(0, count)]
            pltpu.make_async_copy(ref, ref, sem).wait()

    def wait_sends():
        for plane in range(R):
            @pl.when(z == plane)
            def _():
                drain(rowbuf, plane + q - 1, row_send.at[0])
                homed = r == z if plane else False
                for more in (0, 1) if plane else (0,):
                    @pl.when(homed if more else jnp.logical_not(homed))
                    def _():
                        drain(hubbuf, plane * G + q * G - 1 + more * (q - 1), hub_send.at[0])

        pl.when(r >= z)(lambda: drain(rowbuf, R - 1, col_send.at[0]))
        drain(outbox, G * C - 1, msg_send.at[0])

    for copy in own:
        copy.wait()
    pl.semaphore_wait(barrier, (z + 1) * q * G - 1 + jnp.where(r >= z, (R - 1) * q, 0))
    def start(copy):
        copy.start()

    send_near(start)
    send_far(start)
    send_cols(start, range(1, R))
    for dz in range(1, R):
        for dx in range(1, q):
            for dg in range(G):
                homed = jnp.logical_and(z == r, z == dz) if dg == 0 else False

                @pl.when(jnp.logical_and(z >= dz, jnp.logical_not(homed)))
                def _():
                    pl.semaphore_signal(seen, inc=1, device_id=at(z - dz, dx, dg), device_id_type=MESH)

    for h in range(nh // LANES):
        hubcol[h * LANES:(h + 1) * LANES, :] = jnp.transpose(
            jnp.broadcast_to(ids_ref[h:h + 1, :], (LANES, LANES)))

    def hub_hits(base):
        return hubcol[...] == base + lax.broadcasted_iota(jnp.int32, (nh, LANES), 1)

    def light_lanes(t, carry):
        hit = jnp.max(jnp.where(hub_hits(t * LANES), 1, 0), axis=0, keepdims=True)
        keep[pl.ds(t, 1), :] = hit - 1
        return carry

    tiles = bc // LANES
    lax.fori_loop(0, C * tiles, light_lanes, 0)

    def keep_of(block, first=0, count=tiles):
        return jnp.concatenate([keep[pl.ds(block * tiles + first + t, 1), :] for t in range(count)], axis=1)

    part = pl.ds(pl.multiple_of(g * pc, LANES), pc)

    def wait_cols(plane):
        pl.when(plane != r)(lambda: drain(rowbuf, 1, col_recv.at[plane]))

    def part_keep(tx):
        return keep_of(z * q + tx, g * (pc // LANES), pc // LANES)

    def lanes_of(tx):
        return pl.ds(pl.multiple_of(tx * pc, LANES), pc)

    def load_light(tx):
        kept = part_keep(tx)
        for w in range(bw):
            abuf[nh + 32 * w:nh + 32 * w + 32, lanes_of(tx)] = spread(
                rowbuf[z * q + tx, w:w + 1, part] & kept, 1.0).astype(BIT)

    def load_hubs(tx):
        kept = part_keep(tx)
        for j in range(G):
            for w in range(hw):
                lo = 32 * (j * hw + w)
                abuf[lo:lo + 32, lanes_of(tx)] = spread(
                    hubbuf[j * C + z * q + tx, w:w + 1, part] & kept, 1.0).astype(BIT)

    def load_b(plane, base, hubs):
        first = x * wq - x * wq // 8 * 8
        weight = jnp.where(plane == z, 1.0, 2.0)
        for tx in range(q):
            for w in range(wq):
                bits = colbuf[plane, tx, pl.ds(first + w, 1), part]
                bbuf[base + 32 * w:base + 32 * w + 32, tx * pc:(tx + 1) * pc] = spread(bits, weight).astype(BIT)
        if hubs:
            bbuf[base:base + bc, q * pc:] = hub_rows(plane * q + x, 2.0)

    def hub_rows(block, value):
        return jnp.transpose(jnp.concatenate(
            [spread(hubbuf[g * C + block, w:w + 1, :], value) for w in range(hw)], axis=0)).astype(BIT)

    def load_home():
        @pl.when(r > 0)
        def _():
            drain(hubbuf, G, hub_recv.at[2 + r])
            drain(hubbuf, q - 1, hub_recv.at[2])

        for k in range(q):
            abuf[nh + k * bc:nh + (k + 1) * bc, q * pc:] = hub_rows(r * q + k, 1.0)

    def multiply(planes, base, hubs):
        wide = q * pc + (ng if hubs else 0)
        for n, plane in enumerate(planes):
            load_b(plane, n * bc, hubs)
        deep = len(planes) * bc
        product[:, base:base + deep] = lax.dot_general(
            abuf[:, :wide], bbuf[:deep, :wide], (((1,), (1,)), ((), ())), preferred_element_type=jnp.float32)

    def over_lanes(row):
        return functools.reduce(jnp.add, [row[:, t:t + LANES] for t in range(0, row.shape[1], LANES)])

    def close(plane, base, start, stop):
        k = plane * q + x
        kept = keep_of(k)
        words = [(j, w) for j in range(G) for w in range(hw)] + [(G, w) for w in range(bw)]
        for n in range(start // 32, stop // 32):
            j, w = words[n]
            bits = (hubbuf[j * C + k, w:w + 1, :] if j < G else rowbuf[k, w:w + 1, :]) & kept
            at = slice(32 * n, 32 * n + 32)
            wsum[at, :] += over_lanes(spread(bits, product[at, base:base + bc]))

    wsum[...] = jnp.zeros_like(wsum)
    load_light(x)
    for t in range(rows // LANES):
        lanes = slice(t * LANES, (t + 1) * LANES)
        hits = jnp.where(hub_hits(r * rows + t * LANES), 1.0, 0.0)
        owner[:, lanes] = hits
        light[:, lanes] = 1.0 - jnp.sum(hits, axis=0, keepdims=True)

    drain(hubbuf, G - 1, hub_recv.at[0])
    load_hubs(x)

    kept = part_keep(x)
    hub_deg = jnp.sum(jnp.concatenate([
        over_lanes(spread(hubbuf[j * C + c, w:w + 1, part] & kept, 1.0)) for j in range(G) for w in range(hw)],
        axis=0), axis=1, keepdims=True)

    def turn(matrix):
        ones = jnp.ones((8, matrix.shape[1]), matrix.dtype)
        return lax.dot_general(
            ones, matrix, (((1,), (1,)), ((), ())), preferred_element_type=jnp.float32)[:1, :]

    def owned(row, column, start=0):
        lanes = slice(start, start + row.shape[1])
        return light[:, lanes] * row + jnp.sum(owner[:, lanes] * column, axis=0, keepdims=True)

    def post(row, value, owners=range(C)):
        for slot in range(G * C):
            to = slot % C
            if to not in owners:
                continue
            outbox[slot, row:row + 1, :per] = value[:, to * per:(to + 1) * per]

    deg_row = owned(turn(abuf[nh:, lanes_of(x)]), hub_deg)
    post(1, deg_row)

    drain(hubbuf, (q - 1) * G, hub_recv.at[1])
    for dx in range(1, q):
        other = (x + dx) % q
        load_hubs(other)
    drain(rowbuf, q - 1, row_recv.at[0])
    for dx in range(1, q):
        other = (x + dx) % q
        load_light(other)

    base = x * wq // 8 * 8
    for tx in range(q):
        colbuf[r, tx] = rowbuf[z * q + tx, pl.ds(pl.multiple_of(base, 8), colbuf.shape[2]), :]

    @pl.when(z == 0)
    def _():
        abuf[:nh, q * pc:] = jnp.zeros((nh, ng), BIT)
        load_home()

        @pl.when(x == 0)
        def _():
            extra = light[...] * jnp.concatenate([
                jnp.sum(functools.reduce(jnp.add, [
                    spread(hubbuf[g * C + r * q + k, w:w + 1, :], 1.0) for w in range(hw)]), axis=0, keepdims=True)
                for k in range(q)], axis=1)
            post(1, deg_row + extra)

    def wait_hubs(plane):
        homed = jnp.logical_and(z == 0, plane == r)

        @pl.when(jnp.logical_and(plane > z, jnp.logical_not(homed)))
        def _():
            drain(hubbuf, G, hub_recv.at[2 + plane - z])

    def wait_row(plane):
        drain(rowbuf, 1, row_recv.at[plane - z])

    def meet_row(plane):
        pl.when(plane > z)(functools.partial(wait_row, plane))

    odd = (R - z) % 2
    last = R - 1

    @pl.when(odd == 1)
    def _():
        wait_cols(z)

        @pl.when(z < last)
        def _():
            multiply([z], bc, R % 2 == 1)
            close(z, bc, 0, nh + rows)

        @pl.when(z == last)
        def _():
            multiply([z], bc, R == 1)

    def pair(n, carry):
        planes = [z + odd + 2 * n, z + odd + 2 * n + 1]
        for plane in planes:
            wait_cols(plane)
            wait_hubs(plane)
        meet_row(planes[0])
        for hubs, mine in [(True, z == 0), (False, z > 0)]:
            @pl.when(mine)
            def _():
                multiply(planes, 0, hubs)
                close(planes[0], 0, 0, nh + rows)

        wait_row(planes[1])

        @pl.when(planes[1] < last)
        def _():
            close(planes[1], bc, 0, nh + rows)

        return carry

    lax.fori_loop(0, (R - z) // 2, pair, 0)
    close(last, bc, 0, front)
    largest = 2 * (q * pc + ng) * R * (bc // LANES)

    def row_sums(start, stop):
        rest = wsum[start:stop, :]
        row = jnp.zeros((1, stop - start), jnp.float32)
        for _ in range(-(-largest.bit_length() // 8)):
            upper = rest.astype(jnp.bfloat16)
            row = row + turn(upper)
            rest = rest - upper.astype(jnp.float32)
        return row

    def message(slot):
        return pltpu.make_async_remote_copy(
            src_ref=outbox.at[slot], dst_ref=inbox.at[me], send_sem=msg_send.at[0], recv_sem=msg_recv.at[0],
            device_id=(r, slot % C, slot // C), device_id_type=MESH)

    def messages(act, owners):
        for slot in range(G * C):
            if slot % C in owners:
                @pl.when(slot != me)
                def _():
                    act(message(slot))

    hub_tri = jnp.sum(wsum[:nh, :], axis=1, keepdims=True)
    lead_row = owned(row_sums(nh, front), hub_tri)
    for slot in range(0, G * C, C):
        outbox[slot, 0:1, :per] = lead_row[:, :per]
    messages(start, range(1))

    close(last, bc, front, nh + rows)
    later = range(1, C)
    post(0, jnp.concatenate([lead_row, owned(row_sums(front, nh + rows), hub_tri, lead)], axis=1), later)

    @pl.when(z < R - 1)
    def _():
        pl.semaphore_wait(seen, (R - 1 - z) * (q - 1) * G - jnp.where(jnp.logical_and(z == 0, r > 0), q - 1, 0))

    messages(start, later)
    wait_sends()
    drain(inbox, G * C - 1, msg_recv.at[0])
    tri = outbox[me, 0:1, :]
    deg = outbox[me, 1:2, :]
    for d in range(1, G * C):
        slot = (me + d) % (G * C)
        tri = tri + inbox[slot, 0:1, :]
        deg = deg + inbox[slot, 1:2, :]
    out_ref[...] = (0.5 * tri / (1.0 + deg))[:, :per]


def body(light_bits, hub_bits, hub_ids):
    R, C, G = lax.axis_size("rows"), lax.axis_size("cols"), lax.axis_size("hub")
    bw, bc = light_bits.shape
    hw = hub_bits.shape[0]
    nh = hub_ids.shape[0]
    rows, pc = 32 * bw, bc // G
    per = rows // C
    q = C // R
    size = size_of(bw // q, q)
    dma = pltpu.SemaphoreType.DMA
    hbm = pl.BlockSpec(memory_space=pltpu.HBM)
    buffers = [
        ((nh // LANES, LANES), jnp.int32),
        ((C, bw, bc), jnp.int32),
        ((R, q, size, bc), jnp.int32),
        ((G * C, hw, bc), jnp.int32),
        ((C * bc // LANES, LANES), jnp.int32),
        ((nh, LANES), jnp.int32),
        ((rows + nh, q * pc + nh // G), BIT),
        ((2 * bc, q * pc + nh // G), BIT),
        ((nh, rows), jnp.float32),
        ((1, rows), jnp.float32),
        ((rows + nh, 2 * bc), jnp.float32),
        ((rows + nh, LANES), jnp.float32),
        ((G * C, 2, LANES), jnp.float32),
        ((G * C, 2, LANES), jnp.float32),
    ]
    held = sum(math.prod(shape) * jnp.dtype(dtype).itemsize for shape, dtype in buffers)
    held += 8 * (rows + nh) * bc
    out = pl.pallas_call(
        functools.partial(kernel, R, C, G),
        out_shape=jax.ShapeDtypeStruct((1, per), jnp.float32),
        in_specs=[hbm, hbm, hbm],
        out_specs=pl.BlockSpec(memory_space=pltpu.VMEM),
        scratch_shapes=[pltpu.VMEM(shape, dtype) for shape, dtype in buffers] + [
            dma((3,)), dma((1,)), dma((R,)), dma((1,)), dma((R,)),
            dma((1,)), dma((R + 2,)), dma((1,)), dma((1,)), pltpu.SemaphoreType.REGULAR,
        ],
        compiler_params=pltpu.CompilerParams(
            collective_id=0, has_side_effects=True, vmem_limit_bytes=held + 12 * 1024 * 1024),
    )(*(pltpu.with_memory_space_constraint(x, pltpu.HBM)
        for x in (light_bits, hub_bits, hub_ids.reshape(nh // LANES, LANES))))
    return out.reshape(per)


def solution(mesh):
    return jax.shard_map(
        body,
        mesh=mesh,
        in_specs=(P("rows", "cols"), P("hub", "cols"), P()),
        out_specs=P(("rows", "cols")),
        check_vma=False,
    )
```

```python
import functools
import math

import jax
import jax.numpy as jnp
from jax import lax
from jax.experimental import pallas as pl
from jax.experimental.pallas import tpu as pltpu
from jax.sharding import PartitionSpec as P

LANES = 128
BIT = jnp.float8_e4m3fn
MESH = pl.DeviceIdType.MESH


def spread(row, value, other=0.0):
    masks = jnp.left_shift(jnp.int32(1), lax.broadcasted_iota(jnp.int32, (32, row.shape[1]), 0))
    return jnp.where((jnp.broadcast_to(row, masks.shape) & masks) != 0, value, other)


def pieces(wq, x):
    cuts = [x * wq] + [t for t in range(8, (x + 1) * wq, 8) if t > x * wq] + [(x + 1) * wq]
    parts = []
    for lo, hi in zip(cuts, cuts[1:]):
        if parts and lo % 8 == 0 and hi % 8 == 0 and parts[-1][0] % 8 == 0 and sum(parts[-1]) == lo:
            parts[-1] = (parts[-1][0], hi - parts[-1][0])
        else:
            parts.append((lo, hi - lo))
    return parts


def size_of(wq, q):
    return max(-(-(x + 1) * wq // 8) * 8 - x * wq // 8 * 8 for x in range(q))


def kernel(
    R, C, G,
    light_hbm, hub_hbm, ids_hbm, out_ref,
    ids_ref, rowbuf, colbuf, hubbuf, keep, hubcol, abuf, bbuf, owner, light, product, wsum, outbox, inbox,
    local_sem, row_send, row_recv, col_send, col_recv, hub_send, hub_recv, msg_send, msg_recv, seen,
):
    r, c, g = lax.axis_index("rows"), lax.axis_index("cols"), lax.axis_index("hub")
    _, bw, bc = rowbuf.shape
    hw = hubbuf.shape[1]
    pc = bc // G
    q = C // R
    z, x = c // q, c % q
    rows = 32 * bw
    wq = bw // q
    ng = 32 * hw
    nh = ng * G
    per = rows // C
    lead = -(-per // LANES) * LANES
    front = nh + lead
    me = g * C + c

    own = [
        pltpu.make_async_copy(light_hbm, rowbuf.at[c], local_sem.at[0]),
        pltpu.make_async_copy(hub_hbm, hubbuf.at[me], local_sem.at[1]),
        pltpu.make_async_copy(ids_hbm, ids_ref, local_sem.at[2]),
    ]
    for copy in own:
        copy.start()

    def at(plane, dx, dg=0):
        return (r, plane * q + (x + dx) % q, (g + dg) % G)

    barrier = pltpu.get_barrier_semaphore()

    def greet(device):
        pl.semaphore_signal(barrier, inc=1, device_id=device, device_id_type=MESH)

    for dz in range(R):
        @pl.when(z + dz < R)
        def _():
            for dx in range(q):
                for dg in range(G):
                    if dz or dx or dg:
                        greet(at(z + dz, dx, dg))
    for dr in range(1, R):
        @pl.when((r + dr) % R >= z)
        def _():
            for dx in range(q):
                greet(((r + dr) % R, z * q + dx, g))

    def row_copy(dz, dx):
        return pltpu.make_async_remote_copy(
            src_ref=rowbuf.at[c], dst_ref=rowbuf.at[c], send_sem=row_send.at[0], recv_sem=row_recv.at[dz],
            device_id=at(z - dz, dx), device_id_type=MESH)

    def hub_copy(dz, dx, dg):
        return pltpu.make_async_remote_copy(
            src_ref=hubbuf.at[me], dst_ref=hubbuf.at[me], send_sem=hub_send.at[0],
            recv_sem=hub_recv.at[1 + dz if dz else 0 if dx else R + 1], device_id=at(z - dz, dx, dg), device_id_type=MESH)

    def homing(dx):
        return pltpu.make_async_remote_copy(
            src_ref=hubbuf.at[me], dst_ref=hubbuf.at[me], send_sem=hub_send.at[0],
            recv_sem=hub_recv.at[1], device_id=at(0, dx), device_id_type=MESH)

    def col_copies(to, tx):
        base = tx * wq // 8 * 8
        return [
            pltpu.make_async_remote_copy(
                src_ref=rowbuf.at[c, pl.ds(lo, size), :], dst_ref=colbuf.at[r, x, pl.ds(lo - base, size), :],
                send_sem=col_send.at[0], recv_sem=col_recv.at[r],
                device_id=(to, z * q + tx, g), device_id_type=MESH)
            for lo, size in pieces(wq, tx)]

    def send_cols(act, targets):
        @pl.when(r >= z)
        def _():
            for to in targets:
                @pl.when(r != to)
                def _():
                    for tx in range(q):
                        for copy in col_copies(to, tx):
                            act(copy)

    def send_near(act):
        @pl.when(jnp.logical_and(z == r, z > 0))
        def _():
            for dx in range(1, q):
                act(homing(dx))

        send_cols(act, range(1))
        for dx in range(q):
            for dg in range(G):
                if dx or dg:
                    act(hub_copy(0, dx, dg))
        for dx in range(1, q):
            act(row_copy(0, dx))

    def send_far(act):
        for dz in [1] + list(range(R - 1, 1, -1)):
            @pl.when(z >= dz)
            def _():
                for dg in range(G):
                    act(hub_copy(dz, 0, dg))
                act(row_copy(dz, 0))

    def drain(buffer, count, sem):
        if count:
            ref = buffer.at[pl.ds(0, count)]
            pltpu.make_async_copy(ref, ref, sem).wait()

    def wait_sends():
        for plane in range(R):
            @pl.when(z == plane)
            def _():
                drain(rowbuf, plane + q - 1, row_send.at[0])
                homed = r == z if plane else False
                for more in (0, 1) if plane else (0,):
                    @pl.when(homed if more else jnp.logical_not(homed))
                    def _():
                        drain(hubbuf, plane * G + q * G - 1 + more * (q - 1), hub_send.at[0])

        pl.when(r >= z)(lambda: drain(rowbuf, R - 1, col_send.at[0]))
        drain(outbox, G * C - 1, msg_send.at[0])

    for copy in own:
        copy.wait()
    pl.semaphore_wait(barrier, (z + 1) * q * G - 1 + jnp.where(r >= z, (R - 1) * q, 0))
    def start(copy):
        copy.start()

    send_near(start)
    send_far(start)
    send_cols(start, range(1, R))
    for dz in range(1, R):
        for dx in range(1, q):
            for dg in range(G):
                homed = jnp.logical_and(z == r, z == dz) if dg == 0 else False

                @pl.when(jnp.logical_and(z >= dz, jnp.logical_not(homed)))
                def _():
                    pl.semaphore_signal(seen, inc=1, device_id=at(z - dz, dx, dg), device_id_type=MESH)

    for h in range(nh // LANES):
        hubcol[h * LANES:(h + 1) * LANES, :] = jnp.transpose(
            jnp.broadcast_to(ids_ref[h:h + 1, :], (LANES, LANES)))

    def hub_hits(base):
        return hubcol[...] == base + lax.broadcasted_iota(jnp.int32, (nh, LANES), 1)

    def light_lanes(t, carry):
        hit = jnp.max(jnp.where(hub_hits(t * LANES), 1, 0), axis=0, keepdims=True)
        keep[pl.ds(t, 1), :] = hit - 1
        return carry

    tiles = bc // LANES
    lax.fori_loop(0, C * tiles, light_lanes, 0)

    def keep_of(block, first=0, count=tiles):
        return jnp.concatenate([keep[pl.ds(block * tiles + first + t, 1), :] for t in range(count)], axis=1)

    part = pl.ds(pl.multiple_of(g * pc, LANES), pc)

    def wait_cols(plane):
        pl.when(plane != r)(lambda: drain(rowbuf, 1, col_recv.at[plane]))

    def part_keep(tx):
        return keep_of(z * q + tx, g * (pc // LANES), pc // LANES)

    def lanes_of(tx):
        return pl.ds(pl.multiple_of(tx * pc, LANES), pc)

    def load_light(tx):
        kept = part_keep(tx)
        for w in range(bw):
            abuf[nh + 32 * w:nh + 32 * w + 32, lanes_of(tx)] = spread(
                rowbuf[z * q + tx, w:w + 1, part] & kept, 1.0).astype(BIT)

    def load_hubs(tx):
        kept = part_keep(tx)
        for j in range(G):
            for w in range(hw):
                lo = 32 * (j * hw + w)
                abuf[lo:lo + 32, lanes_of(tx)] = spread(
                    hubbuf[j * C + z * q + tx, w:w + 1, part] & kept, 1.0).astype(BIT)

    def load_b(plane, base, hubs):
        first = x * wq - x * wq // 8 * 8
        weight = jnp.where(plane == z, 1.0, 2.0)
        for tx in range(q):
            for w in range(wq):
                bits = colbuf[plane, tx, pl.ds(first + w, 1), part]
                bbuf[base + 32 * w:base + 32 * w + 32, tx * pc:(tx + 1) * pc] = spread(bits, weight).astype(BIT)
        if hubs:
            bbuf[base:base + bc, q * pc:] = hub_rows(plane * q + x, 2.0)

    def hub_rows(block, value):
        return jnp.transpose(jnp.concatenate(
            [spread(hubbuf[g * C + block, w:w + 1, :], value) for w in range(hw)], axis=0)).astype(BIT)

    def load_home():
        @pl.when(r > 0)
        def _():
            drain(hubbuf, G, hub_recv.at[1 + r])
            drain(hubbuf, q - 1, hub_recv.at[1])

        for k in range(q):
            abuf[nh + k * bc:nh + (k + 1) * bc, q * pc:] = hub_rows(r * q + k, 1.0)

    def multiply(planes, base, hubs):
        wide = q * pc + (ng if hubs else 0)
        for n, plane in enumerate(planes):
            load_b(plane, n * bc, hubs)
        deep = len(planes) * bc
        product[:, base:base + deep] = lax.dot_general(
            abuf[:, :wide], bbuf[:deep, :wide], (((1,), (1,)), ((), ())), preferred_element_type=jnp.float32)

    def over_lanes(row):
        return functools.reduce(jnp.add, [row[:, t:t + LANES] for t in range(0, row.shape[1], LANES)])

    def close(plane, base, start, stop):
        k = plane * q + x
        kept = keep_of(k)
        words = [(j, w) for j in range(G) for w in range(hw)] + [(G, w) for w in range(bw)]
        for n in range(start // 32, stop // 32):
            j, w = words[n]
            bits = (hubbuf[j * C + k, w:w + 1, :] if j < G else rowbuf[k, w:w + 1, :]) & kept
            at = slice(32 * n, 32 * n + 32)
            wsum[at, :] += over_lanes(spread(bits, product[at, base:base + bc]))

    wsum[...] = jnp.zeros_like(wsum)
    load_light(x)
    for t in range(rows // LANES):
        lanes = slice(t * LANES, (t + 1) * LANES)
        hits = jnp.where(hub_hits(r * rows + t * LANES), 1.0, 0.0)
        owner[:, lanes] = hits
        light[:, lanes] = 1.0 - jnp.sum(hits, axis=0, keepdims=True)

    if G > 1:
        drain(hubbuf, G - 1, hub_recv.at[R + 1])
    load_hubs(x)

    kept = part_keep(x)
    hub_deg = jnp.sum(jnp.concatenate([
        over_lanes(spread(hubbuf[j * C + c, w:w + 1, part] & kept, 1.0)) for j in range(G) for w in range(hw)],
        axis=0), axis=1, keepdims=True)

    def turn(matrix):
        ones = jnp.ones((8, matrix.shape[1]), matrix.dtype)
        return lax.dot_general(
            ones, matrix, (((1,), (1,)), ((), ())), preferred_element_type=jnp.float32)[:1, :]

    def owned(row, column, start=0):
        lanes = slice(start, start + row.shape[1])
        return light[:, lanes] * row + jnp.sum(owner[:, lanes] * column, axis=0, keepdims=True)

    def post(row, value, owners=range(C)):
        for slot in range(G * C):
            to = slot % C
            if to not in owners:
                continue
            outbox[slot, row:row + 1, :per] = value[:, to * per:(to + 1) * per]

    deg_row = owned(turn(abuf[nh:, lanes_of(x)]), hub_deg)
    post(1, deg_row)

    drain(hubbuf, (q - 1) * G, hub_recv.at[0])
    for dx in range(1, q):
        other = (x + dx) % q
        load_hubs(other)
    drain(rowbuf, q - 1, row_recv.at[0])
    for dx in range(1, q):
        other = (x + dx) % q
        load_light(other)

    base = x * wq // 8 * 8
    for tx in range(q):
        colbuf[r, tx] = rowbuf[z * q + tx, pl.ds(pl.multiple_of(base, 8), colbuf.shape[2]), :]

    @pl.when(z == 0)
    def _():
        abuf[:nh, q * pc:] = jnp.zeros((nh, ng), BIT)
        load_home()

        @pl.when(x == 0)
        def _():
            extra = light[...] * jnp.concatenate([
                jnp.sum(functools.reduce(jnp.add, [
                    spread(hubbuf[g * C + r * q + k, w:w + 1, :], 1.0) for w in range(hw)]), axis=0, keepdims=True)
                for k in range(q)], axis=1)
            post(1, deg_row + extra)

    def wait_hubs(plane):
        homed = jnp.logical_and(z == 0, plane == r)

        @pl.when(jnp.logical_and(plane > z, jnp.logical_not(homed)))
        def _():
            drain(hubbuf, G, hub_recv.at[1 + plane - z])

    def wait_row(plane):
        drain(rowbuf, 1, row_recv.at[plane - z])

    def meet_row(plane):
        pl.when(plane > z)(functools.partial(wait_row, plane))

    odd = (R - z) % 2
    last = R - 1

    @pl.when(odd == 1)
    def _():
        wait_cols(z)

        @pl.when(z < last)
        def _():
            multiply([z], bc, R % 2 == 1)
            close(z, bc, 0, nh + rows)

        @pl.when(z == last)
        def _():
            multiply([z], bc, R == 1)

    def pair(n, carry):
        planes = [z + odd + 2 * n, z + odd + 2 * n + 1]
        for plane in planes:
            wait_cols(plane)
            wait_hubs(plane)
        meet_row(planes[0])
        more = planes[1] < last

        @pl.when(more)
        def _():
            wait_row(planes[1])

        for hubs, mine in [(True, z == 0), (False, z > 0)]:
            for both in [True, False] if R > (3 if hubs else 5) else [False]:
                @pl.when(jnp.logical_and(mine, more if both else jnp.logical_not(more)))
                def _():
                    multiply(planes, 0, hubs)
                    close(planes[0], 0, 0, nh + rows)
                    if both:
                        close(planes[1], bc, 0, nh + rows)

        @pl.when(jnp.logical_not(more))
        def _():
            wait_row(planes[1])

        return carry

    lax.fori_loop(0, (R - z) // 2, pair, 0)
    pl.when(c == 0)(lambda: close(last, bc, 0, front))
    largest = 2 * (q * pc + ng) * R * (bc // LANES)

    def row_sums(start, stop):
        rest = wsum[start:stop, :]
        row = jnp.zeros((1, stop - start), jnp.float32)
        for _ in range(-(-largest.bit_length() // 8)):
            upper = rest.astype(jnp.bfloat16)
            row = row + turn(upper)
            rest = rest - upper.astype(jnp.float32)
        return row

    def message(slot):
        return pltpu.make_async_remote_copy(
            src_ref=outbox.at[slot], dst_ref=inbox.at[me], send_sem=msg_send.at[0], recv_sem=msg_recv.at[0],
            device_id=(r, slot % C, slot // C), device_id_type=MESH)

    def messages(act, owners):
        for slot in reversed(range(G * C)):
            if slot % C in owners:
                @pl.when(slot != me)
                def _():
                    act(message(slot))

    @pl.when(c > 0)
    def _():
        close(last, bc, 0, front)
        hub_tri = jnp.sum(wsum[:nh, :], axis=1, keepdims=True)
        lead_row = owned(row_sums(nh, front), hub_tri)
        for slot in range(0, G * C, C):
            outbox[slot, 0:1, :per] = lead_row[:, :per]
        messages(start, range(1))

    close(last, bc, front, nh + rows)
    hub_tri = jnp.sum(wsum[:nh, :], axis=1, keepdims=True)
    tri_row = owned(row_sums(nh, nh + rows), hub_tri)
    later = range(1, C)
    post(0, tri_row, later)

    @pl.when(c == 0)
    def _():
        post(0, tri_row, range(1))
        messages(start, range(1))

    @pl.when(z < R - 1)
    def _():
        pl.semaphore_wait(seen, (R - 1 - z) * (q - 1) * G - jnp.where(jnp.logical_and(z == 0, r > 0), q - 1, 0))

    messages(start, later)
    wait_sends()
    drain(inbox, G * C - 1, msg_recv.at[0])
    tri = outbox[me, 0:1, :]
    deg = outbox[me, 1:2, :]
    for d in range(1, G * C):
        slot = (me + d) % (G * C)
        tri = tri + inbox[slot, 0:1, :]
        deg = deg + inbox[slot, 1:2, :]
    out_ref[...] = (0.5 * tri / (1.0 + deg))[:, :per]


def body(light_bits, hub_bits, hub_ids):
    R, C, G = lax.axis_size("rows"), lax.axis_size("cols"), lax.axis_size("hub")
    bw, bc = light_bits.shape
    hw = hub_bits.shape[0]
    nh = hub_ids.shape[0]
    rows, pc = 32 * bw, bc // G
    per = rows // C
    q = C // R
    size = size_of(bw // q, q)
    dma = pltpu.SemaphoreType.DMA
    hbm = pl.BlockSpec(memory_space=pltpu.HBM)
    buffers = [
        ((nh // LANES, LANES), jnp.int32),
        ((C, bw, bc), jnp.int32),
        ((R, q, size, bc), jnp.int32),
        ((G * C, hw, bc), jnp.int32),
        ((C * bc // LANES, LANES), jnp.int32),
        ((nh, LANES), jnp.int32),
        ((rows + nh, q * pc + nh // G), BIT),
        ((2 * bc, q * pc + nh // G), BIT),
        ((nh, rows), jnp.float32),
        ((1, rows), jnp.float32),
        ((rows + nh, 2 * bc), jnp.float32),
        ((rows + nh, LANES), jnp.float32),
        ((G * C, 2, LANES), jnp.float32),
        ((G * C, 2, LANES), jnp.float32),
    ]
    held = sum(math.prod(shape) * jnp.dtype(dtype).itemsize for shape, dtype in buffers)
    held += 8 * (rows + nh) * bc
    out = pl.pallas_call(
        functools.partial(kernel, R, C, G),
        out_shape=jax.ShapeDtypeStruct((1, per), jnp.float32),
        in_specs=[hbm, hbm, hbm],
        out_specs=pl.BlockSpec(memory_space=pltpu.VMEM),
        scratch_shapes=[pltpu.VMEM(shape, dtype) for shape, dtype in buffers] + [
            dma((3,)), dma((1,)), dma((R,)), dma((1,)), dma((R,)),
            dma((1,)), dma((R + 1 + (G > 1),)), dma((1,)), dma((1,)), pltpu.SemaphoreType.REGULAR,
        ],
        compiler_params=pltpu.CompilerParams(
            collective_id=0, has_side_effects=True, vmem_limit_bytes=held + 12 * 1024 * 1024),
    )(*(pltpu.with_memory_space_constraint(x, pltpu.HBM)
        for x in (light_bits, hub_bits, hub_ids.reshape(nh // LANES, LANES))))
    return out.reshape(per)


def solution(mesh):
    return jax.shard_map(
        body,
        mesh=mesh,
        in_specs=(P("rows", "cols"), P("hub", "cols"), P()),
        out_specs=P(("rows", "cols")),
        check_vma=False,
    )
```
